32 devices in a mesh: state: 2 (over x), bond: 16 (over z, y, core).
Axes of the slice: x: 2, y: 2, z: 4, core: 2. Of those that a mesh axis runs over, the one named last changes fastest.
Arguments:
- intersect_left: bfloat16 [2, 2048, 2048], P('state', 'bond'), may hold values from -0.125 to 0.125
- stored_block: bfloat16 [2, 4, 2048, 2048], P('state', None, 'bond'), may hold values from -6 to 6
- stored_site: bfloat16 [2, 2, 2048, 2048], P('state', None, 'bond'), may hold values from -6 to 6
- current_site: bfloat16 [2048, 2, 2048], P('bond', None, 'state'), may hold values from -0.09375 to 0.09375
- current_block: bfloat16 [4, 2048, 2048], P(None, 'bond', 'state'), may hold values from -6 to 6
- penalty_weight: float32 [2], replicated, may hold values from 0.5 to 4
Outputs:
- penalized: float32 [4, 2048, 2048], P(None, 'bond', 'state')
- intersect_next: bfloat16 [2, 2048, 2048], P('state', 'bond')
The draws below stay inside these ranges and needn't reach their ends.
All inputs are finite; a program needn't handle non-finite values.
Results may differ from the reference program's by a relative error of at most 0.0055.
Values may be sent and summed in bfloat16 or wider, within the bound.
A program may use at most 64 MiB of HBM per device.

```python
import math
import jax
import jax.numpy as jnp

D = 2048
PHYS = 2
Q = 4
STATES = 2


def level_of(rng, dims, pieces, least, high):
    def one(axis_at, shards_of):
        draws = jax.random.uniform(jax.random.fold_in(jax.random.fold_in(rng, 6), axis_at), (shards_of,), jnp.float32, least / len(pieces), high / len(pieces))
        return jnp.repeat(jnp.exp(draws), dims[axis_at] // shards_of).reshape((-1,) + (1,) * (len(dims) - axis_at - 1))

    factor_of = one(*pieces[0])
    for cut in pieces[1:]:
        factor_of = factor_of * one(*cut)
    return factor_of


def normal_values(key, dims, scale, limit, split=(), kind=jnp.bfloat16):
    result = scale * jax.random.normal(key, dims, jnp.float32)
    if split:
        result = result * level_of(key, dims, split, -0.22, 0.18)
    return jnp.clip(result, -limit, limit).astype(kind)


def setup_inputs(seed: int = 0) -> dict:
    seeds = jax.random.split(jax.random.key(seed), 7)
    return {
        "intersect_left": normal_values(seeds[0], (STATES, D, D), D ** -0.5, 0.125, ((0, 2), (1, 16))),
        "stored_block": normal_values(seeds[1], (STATES, Q, D, D), 1.0, 6.0, ((0, 2), (2, 16))),
        "stored_site": normal_values(seeds[2], (STATES, PHYS, D, D), 1.0, 6.0, ((0, 2), (2, 16))),
        "current_site": normal_values(seeds[3], (D, PHYS, D), (PHYS * D) ** -0.5, 0.09375, ((0, 16), (2, 2))),
        "current_block": normal_values(seeds[4], (Q, D, D), 1.0, 6.0, ((1, 16), (2, 2))),
        "penalty_weight": jnp.clip(jnp.exp(jax.random.uniform(seeds[5], (STATES,), jnp.float32, math.log(0.5), math.log(4.0))), 0.5, 4.0),
    }


def reference(intersect_left, stored_block, stored_site, current_site, current_block, penalty_weight):
    block_wide = current_block.astype(jnp.float32)
    site_wide = current_site.astype(jnp.float32)
    penalized = block_wide
    grown_list = []
    for index in range(STATES):
        env_turned = intersect_left[index].T
        projected = jnp.dot(stored_block[index].reshape(Q * D, D), env_turned, preferred_element_type=jnp.float32).reshape(Q, D, D)
        intersect = jnp.sum(projected * block_wide) / (PHYS * D)
        penalized = penalized + (penalty_weight[index] * intersect) * projected
        moved = jnp.dot(stored_site[index].reshape(PHYS * D, D), env_turned, preferred_element_type=jnp.float32).astype(jnp.bfloat16)
        moved = moved.reshape(PHYS, D, D).astype(jnp.float32)
        grown = jnp.einsum("asf,sea->fe", site_wide, moved).astype(jnp.bfloat16)
        grown_list.append(grown)
    return penalized, jnp.stack(grown_list)
```

```python
import functools

import jax
import jax.numpy as jnp
from jax import lax
from jax.experimental import pallas as pl
from jax.experimental.pallas import tpu as pltpu
from jax.sharding import PartitionSpec as P

MESH = pl.DeviceIdType.MESH
CORES = 2
TILE = 256
PARTS = 2


def both(*conds):
    return functools.reduce(jnp.logical_and, conds)


def kernel(
    states, bonds, rows_y, fch,
    env_hbm, block_hbm, site_hbm, grow_hbm, current_hbm, weight_ref,
    pen_hbm, next_hbm,
    ebuf, abuf, stored, cbuf, psend, precv, mown, mbuf, acc, part, prt, nsend, nbuf, pen, iplane, iline, istate, line,
    local_sem, out_sem, e_send, e_recv, a_send, a_recv, p_send, p_recv, my_send, my_recv, mx_send, mx_recv,
    c_send, c_recv, i_send, i_recv, t_send, t_recv, r_send, r_recv, n_send, n_recv,
):
    nc, ny = CORES, rows_y
    nz = bonds // (nc * ny)
    hr, width = ebuf.shape[2:]
    rows = hr * PARTS
    pairs, w = block_hbm.shape[:2]
    phys = site_hbm.shape[0]
    fwidth = grow_hbm.shape[1] // phys
    nch = fwidth // fch
    bpc = fch // w
    fbs = fwidth // w
    mine = fbs // ny
    cell = nc * rows
    per_group = TILE // rows
    tpp = ny * cell // TILE
    cpt = TILE // cell
    groups = width // TILE
    gpp = groups // states
    count = states * bonds
    ecols = states * ny * w
    direct = w % 128 == 0
    piece = phys * cell

    k = lax.axis_index("state")
    me = lax.axis_index("bond")
    c = lax.rem(me, nc)
    y = lax.rem(lax.div(me, nc), ny)
    z = lax.div(me, nc * ny)
    flat = k * bonds + me
    near = ny * nc
    slices = PARTS * tpp

    def slot(zz, yy, cc):
        return (zz * ny + yy) * nc + cc

    sib = slot(z, y, 1 - c)

    def column_of(h, q):
        if direct:
            return (h // nc * ny + q) * nc + h % nc
        return h * bpc + q

    e_load = pltpu.make_async_copy(env_hbm, ebuf.at[me], local_sem.at[0])
    e_load.start()
    a_loads = []
    for h in range(nch):
        for s in range(phys):
            for q in range(bpc if direct else 1):
                size = w if direct else fch
                a_loads.append(
                    pltpu.make_async_copy(
                        grow_hbm.at[:, pl.ds(s * fwidth + column_of(h, q) * w, size)],
                        abuf.at[h, z, s, c, :, pl.ds(q * w, size)],
                        local_sem.at[1],
                    )
                )
    for copy in a_loads:
        copy.start()
    loads = []
    for q in range(pairs):
        loads.append(pltpu.make_async_copy(block_hbm.at[q], stored.at[pl.ds(q * w, w)], local_sem.at[2]))
    for s in range(phys):
        loads.append(
            pltpu.make_async_copy(site_hbm.at[s], stored.at[pl.ds((pairs + s) * w, w)], local_sem.at[2])
        )
    for copy in loads:
        copy.start()
    c_loads = [
        pltpu.make_async_copy(
            current_hbm.at[:, :, pl.ds(g * TILE, TILE)], cbuf.at[k * gpp + g], local_sem.at[3]
        )
        for g in range(gpp)
    ]
    for copy in c_loads:
        copy.start()

    barrier = pltpu.get_barrier_semaphore()

    @pl.loop(1, count)
    def _(r):
        peer = lax.rem(flat + r, count)
        pl.semaphore_signal(
            barrier, inc=1, device_id=(lax.div(peer, bonds), lax.rem(peer, bonds)), device_id_type=MESH
        )

    pl.semaphore_wait(barrier, count - 1)

    def remote(src, dst, ss, rs, kk, dest):
        return pltpu.make_async_remote_copy(
            src_ref=src, dst_ref=dst, send_sem=ss, recv_sem=rs, device_id=(kk, dest), device_id_type=MESH
        )

    def act(copy, drain):
        if drain:
            copy.wait_send()
        else:
            copy.start()


    def e_copy(blk, h, dest):
        ref = ebuf.at[blk, h]
        return remote(ref, ref, e_send, e_recv.at[blk, h], k, dest)

    def spread(blk, h, drain):
        @pl.when(y > 0)
        def _():
            act(e_copy(blk, h, slot(z, y - 1, c)), drain)

        @pl.when(y < ny - 1)
        def _():
            act(e_copy(blk, h, slot(z, y + 1, c)), drain)

        act(e_copy(blk, h, sib), drain)

    def column(i, drain=False):
        for h in range(PARTS):
            if i == 0:
                @pl.when(z > 0)
                def _():
                    act(e_copy(me, h, slot(z - 1, y, c)), drain)

                @pl.when(z < nz - 1)
                def _():
                    act(e_copy(me, h, slot(z + 1, y, c)), drain)

                spread(me, h, drain)
                continue
            for sign in (1, -1):
                zz = z - sign * i
                onward = z + sign

                @pl.when(both(zz >= 0, zz < nz))
                def _():
                    blk = slot(zz, y, c)
                    if not drain:
                        e_copy(blk, h, me).wait_recv()

                    @pl.when(both(onward >= 0, onward < nz))
                    def _():
                        act(e_copy(blk, h, slot(onward, y, c)), drain)

                    spread(blk, h, drain)

    def turn(j):
        least = jnp.minimum(z, nz - 1 - z)
        near = (j + 1) // 2
        inner = z - near if j % 2 else z + near
        far = j - least
        outer = jnp.where(z <= nz - 1 - z, z + far, z - far)
        return jnp.where(j <= 2 * least, inner, outer)

    def across(j, drain=False):
        zz = turn(j)
        for h in range(PARTS):
            for u in range(1, ny):
                for sign in (1, -1):
                    yy = y - sign * u
                    onward = y + sign

                    @pl.when(both(yy >= 0, yy < ny))
                    def _():
                        blk = slot(zz, yy, c)
                        if not drain:
                            e_copy(blk, h, me).wait_recv()

                        @pl.when(both(onward >= 0, onward < ny))
                        def _():
                            act(e_copy(blk, h, slot(z, onward, c)), drain)

                        act(e_copy(blk, h, sib), drain)

    def sibling(j):
        zz = turn(j)
        for h in range(PARTS):
            for yy in range(ny):
                e_copy(slot(zz, yy, 1 - c), h, me).wait_recv()


    def a_copy(h, zz, cc, dest):
        ref = abuf.at[h, zz, :, cc]
        return remote(ref, ref, a_send, a_recv.at[h, zz, cc], k, dest)

    def a_own(sign, drain=False):
        @pl.loop(0, nch)
        def _(h):
            act(a_copy(h, z, c, slot(z + sign, y, c)), drain)

    def a_edges(i, drain=False):
        @pl.when(both(z == i, z < nz - 1))
        def _():
            a_own(1, drain)

        @pl.when(both(nz - 1 - z == i, z > 0))
        def _():
            a_own(-1, drain)

    def a_sibling(drain=False):
        @pl.loop(0, nch)
        def _(h):
            act(a_copy(h, z, c, sib), drain)

    def a_pass(h, i, drain=False):
        for sign in (1, -1):
            zz = z - sign * i
            onward = z + sign

            @pl.when(both(zz >= 0, zz < nz, onward >= 0, onward < nz))
            def _():
                if not drain:
                    a_copy(h, zz, c, me).wait_recv()
                act(a_copy(h, zz, c, slot(onward, y, c)), drain)
                act(a_copy(h, zz, c, sib), drain)

    def a_last(h, i, drain=False):
        for sign in (1, -1):
            zz = z - sign * i
            onward = z + sign

            @pl.when(both(zz >= 0, zz < nz, jnp.logical_or(onward < 0, onward >= nz)))
            def _():
                if not drain:
                    a_copy(h, zz, c, me).wait_recv()
                act(a_copy(h, zz, c, sib), drain)

    def a_ready(h):
        for zz in range(nz):
            a_copy(h, zz, 1 - c, me).wait_recv()


    def c_copy(zz, peer):
        ref = cbuf.at[pl.ds(zz * tpp, tpp)]
        return remote(ref, ref, c_send, c_recv, peer, me)

    def owner_of(zz):
        return lax.div(zz * tpp, gpp)

    def share(drain=False):
        zz = turn(nz - 1)

        @pl.when(owner_of(zz) == k)
        def _():
            for other in range(1, states):
                act(c_copy(zz, lax.rem(k + other, states)), drain)


    def p_copy(g, part_of, peer):
        return remote(
            psend.at[g, part_of], precv.at[k, lax.rem(g, gpp), part_of],
            p_send, p_recv.at[k, lax.div(g, tpp)], peer, me,
        )

    def span(zz):
        return pl.ds(pl.multiple_of(zz * piece, 128), piece)

    def my_copy(zz, yy):
        return remote(
            mown.at[zz, yy], mbuf.at[k, y, :, span(zz)], my_send, my_recv.at[zz, y], k, slot(z, yy, c)
        )

    def mx_copy(zz, yy, peer):
        ref = mbuf.at[k, yy, :, span(zz)]
        return remote(ref, ref, mx_send, mx_recv.at[k], peer, me)

    def flat_of(kk, at):
        return precv[kk, at].reshape(pairs * w, TILE).astype(jnp.float32)

    def halves(whole):
        return whole.astype(jnp.bfloat16).reshape(PARTS, pairs * w // PARTS, TILE)

    def tally(kk, g, whole):
        here = cbuf[g].reshape(pairs * w, TILE).astype(jnp.float32)
        line[kk] += jnp.sum((whole * here).reshape(pairs * w // 8, 8, TILE), axis=0)

    def p_wait(j, use):
        zz = turn(j)

        @pl.when(owner_of(zz) == k)
        def _():
            first = lax.rem(zz * tpp, gpp)
            for other in range(1, states):
                peer = lax.rem(k + other, states)
                ref = precv.at[peer, pl.ds(first, tpp)]
                remote(ref, ref, p_send, p_recv.at[peer, zz], peer, me).wait_recv()
                if use:
                    @pl.loop(0, tpp)
                    def _(r):
                        tally(peer, zz * tpp + r, flat_of(peer, first + r))

    def project(j):
        zz = turn(j)

        if j == nz - 1:
            @pl.when(owner_of(zz) != k)
            def _():
                c_copy(zz, k).wait_recv()

        @pl.loop(0, tpp)
        def _(r):
            g = zz * tpp + r
            left = ebuf[pl.ds(g * per_group, per_group)].reshape(TILE, width)
            prod = lax.dot_general(
                stored[...], left, (((1,), (1,)), ((), ())), preferred_element_type=jnp.float32
            )
            for q in range(cpt):
                yy = r * cpt + q
                moved = jnp.concatenate(
                    [
                        prod[(pairs + s) * w : (pairs + s + 1) * w, q * cell : (q + 1) * cell]
                        for s in range(phys)
                    ],
                    axis=1,
                ).astype(jnp.bfloat16)

                @pl.when(yy == y)
                def _():
                    mbuf[k, y, :, span(zz)] = moved
                    for other in range(1, states):
                        mx_copy(zz, y, lax.rem(k + other, states)).start()

                @pl.when(yy != y)
                def _():
                    mown[zz, yy] = moved
                    if j >= nz - 2:
                        my_copy(zz, yy).start()

            whole = prod[: pairs * w]
            owner = lax.div(g, gpp)

            @pl.when(jnp.logical_or(owner == k, j == nz - 1))
            def _():
                tally(k, g, whole)

            @pl.when(owner == k)
            def _():
                precv[k, lax.rem(g, gpp)] = halves(whole)

            @pl.when(owner != k)
            def _():
                psend[g] = halves(whole)

    def hand_over(j, n, drain=False):
        zz = turn(j)
        g = zz * tpp + n // PARTS
        for other in range(1, states):
            peer = lax.rem(k + other, states)

            @pl.when(lax.div(g, gpp) == peer)
            def _():
                act(p_copy(g, n % PARTS, peer), drain)

    def forward(j, drain=False):
        zz = turn(j)
        for u in range(1, ny):
            yy = lax.rem(y + u, ny)
            if not drain:
                ref = mbuf.at[k, yy, :, span(zz)]
                remote(ref, ref, my_send, my_recv.at[zz, yy], k, me).wait_recv()
            for other in range(1, states):
                act(mx_copy(zz, yy, lax.rem(k + other, states)), drain)


    def t_copy(zc, yy):
        return remote(
            part.at[zc, yy], prt.at[zc, y], t_send, t_recv.at[zc, y], k, slot(z, yy, c)
        )

    def grow(h):
        total = jnp.dot(
            mbuf[...].reshape(ecols, nz * piece),
            abuf[h].reshape(nz * piece, fch),
            preferred_element_type=jnp.float32,
        )
        for q in range(bpc):
            if direct:
                zc, yy = h, q
            else:
                fb = h * bpc + q
                zc = lax.div(fb, ny * nc) * nc + lax.rem(fb, nc)
                yy = lax.rem(lax.div(fb, nc), ny)
            block = total[:, q * w : (q + 1) * w]

            @pl.when(yy == y)
            def _():
                acc[zc] = block

            @pl.when(yy != y)
            def _():
                part[zc, yy] = block.astype(jnp.bfloat16)
                t_copy(zc, yy).start()

    def target(kk, zc):
        return slot(kk * (nz // states) + lax.div(zc, nc), y, lax.rem(zc, nc))

    def place(src):
        if direct:
            return next_hbm.at[:, pl.ds(pl.multiple_of(src * w, 128), w)]
        return next_hbm.at[src]


    def n_copy(kk, zc, yy):
        return remote(
            nbuf.at[kk, zc, yy], place(slot(z, yy, c)), n_send, n_recv, k, target(kk, zc)
        )

    def n_local(kk, zc, yy):
        return pltpu.make_async_copy(nbuf.at[kk, zc, yy], place(slot(z, yy, c)), out_sem.at[1])

    def deliver(kk, zc, drain=False):
        stays = target(kk, zc) == me
        for yy in range(ny):
            @pl.when(stays)
            def _():
                if drain:
                    n_local(kk, zc, yy).wait()
                else:
                    n_local(kk, zc, yy).start()

            @pl.when(jnp.logical_not(stays))
            def _():
                act(n_copy(kk, zc, yy), drain)

    def r_copy(kk, zc):
        return remote(nsend.at[kk, zc], nbuf.at[k, zc], r_send, r_recv.at[k, zc], kk, me)

    def finish(zc):
        total = acc[zc]
        for u in range(1, ny):
            yy = lax.rem(y + u, ny)
            ref = prt.at[zc, yy]
            remote(ref, ref, t_send, t_recv.at[zc, yy], k, me).wait_recv()
            total = total + ref[...].astype(jnp.float32)
        for kk in range(states):
            blocks = [
                total[(kk * ny + yy) * w : (kk * ny + yy + 1) * w].T.astype(jnp.bfloat16)
                for yy in range(ny)
            ]

            @pl.when(kk == k)
            def _():
                for yy in range(ny):
                    nbuf[k, zc, yy] = blocks[yy]
                deliver(k, zc)

            @pl.when(kk != k)
            def _():
                for yy in range(ny):
                    nsend[kk, zc, yy] = blocks[yy]
                r_copy(kk, zc).start()

    def pass_on(zc):
        for other in range(1, states):
            kk = lax.rem(k + other, states)
            ref = nbuf.at[kk, zc]
            remote(ref, ref, r_send, r_recv.at[kk, zc], k, me).wait_recv()
            deliver(kk, zc)


    def i_near(u):
        there = lax.rem(lax.rem(me, near) + u, near)
        ref = iplane.at[lax.rem(me, near)]
        return remote(ref, ref, i_send.at[0], i_recv.at[0], k, z * near + there)

    def i_far(u):
        ref = iline.at[z]
        return remote(ref, ref, i_send.at[1], i_recv.at[1], k, slot(lax.rem(z + u, nz), y, c))

    def i_peer(u):
        ref = istate.at[k]
        return remote(ref, ref, i_send.at[2], i_recv.at[2], lax.rem(k + u, states), me)

    stages = ((i_near, near, iplane), (i_far, nz, iline), (i_peer, states, istate))

    def start(n):
        send, number, _ = stages[n]
        for u in range(1, number):
            send(u).start()

    def gathered(n):
        _, number, buf = stages[n]
        rest = buf.at[pl.ds(0, number - 1)]
        remote(rest, rest, i_send.at[n], i_recv.at[n], k, me).wait_recv()

    def overlap(n):
        if n == 0:
            for kk in range(states):
                short = jnp.sum(line[kk], axis=0, keepdims=True)
                total = short[:, :128]
                for at in range(128, TILE, 128):
                    total = total + short[:, at : at + 128]
                iplane[lax.rem(me, near), kk : kk + 1] = total
        elif n == 1:
            gathered(0)
            iline[z] = jnp.sum(iplane[...], axis=0)
        else:
            gathered(1)
            istate[k] = jnp.sum(iline[...], axis=0)
        start(n)

    pen_copies = [
        pltpu.make_async_copy(pen.at[g], pen_hbm.at[:, :, pl.ds(g * TILE, TILE)], out_sem.at[0])
        for g in range(gpp)
    ]

    def penalize():
        gathered(2)
        p_wait(nz - 1, False)
        scale = 1.0 / (phys * width)
        factors = [weight_ref[kk] * (jnp.sum(istate[:, kk]) * scale) for kk in range(states)]
        for g in range(gpp):
            value = cbuf[k * gpp + g].reshape(pairs * w, TILE).astype(jnp.float32)
            for kk in range(states):
                value = value + factors[kk] * flat_of(kk, g)
            pen[g] = value.reshape(pairs, w, TILE)
            pen_copies[g].start()

    line[...] = jnp.zeros_like(line)
    e_load.wait()
    for i in range(nz + 1):
        if i < nz:
            column(i)
            if i == 0:
                for copy in a_loads:
                    copy.wait()
                a_sibling()
            a_edges(i)
            if i == 0:
                for copy in c_loads:
                    copy.wait()
                share()
        if i == nz - 1:
            for j in range(nz - 2):
                for u in range(1, ny):
                    my_copy(turn(j), lax.rem(y + u, ny)).start()
        if i >= 1:
            across(i - 1)
            sibling(i - 1)
            if i == 1:
                for copy in loads:
                    copy.wait()
            project(i - 1)
            if i < nz:
                for n in range(slices - (i == nz - 1)):
                    hand_over(i - 1, n)
        if i == nz - 1:
            @pl.loop(0, nch)
            def _(h):
                a_pass(h, 1)

    for i in range(2, nz):
        @pl.loop(0, nch)
        def _(h):
            a_pass(h, i)

    for j in range(nz):
        forward(j)
        if 1 <= j < nz - 1:
            @pl.loop(0, nch)
            def _(h):
                a_last(h, j)
    for i in range(nz):
        column(i, drain=True)
        across(i, drain=True)
    a_last(0, nz - 1)
    for other in range(1, states):
        peer = lax.rem(k + other, states)
        ref = mbuf.at[peer]
        remote(ref, ref, mx_send, mx_recv.at[peer], peer, me).wait_recv()

    @pl.loop(0, nch)
    def _(h):
        a_ready(h)
        grow(h)

        @pl.when(h == 0)
        def _():
            hand_over(nz - 2, slices - 1)

        for n in range(slices):
            @pl.when(h == n * nch // slices)
            def _():
                hand_over(nz - 1, n)

        @pl.when(h < nch - 1)
        def _():
            a_last(h + 1, nz - 1)

        @pl.when(h == max(nch - 2, 0))
        def _():
            for j in range(nz - 1):
                p_wait(j, True)
            overlap(0)

        if direct:
            @pl.when(h > 1)
            def _():
                finish(h - 2)

        @pl.when(h == nch - 1)
        def _():
            overlap(1)

    for i in range(nz):
        a_edges(i, drain=True)
    a_sibling(drain=True)

    @pl.loop(0, nch)
    def _(h):
        for i in range(1, nz):
            a_pass(h, i, drain=True)
            a_last(h, i, drain=True)

    if direct:
        for h in range(nch - 2, nch):
            finish(h)
            if h < nch - 1:
                overlap(2)
                pass_on(h - nch + 2)
        for h in range(1, nch):
            pass_on(h)
    else:
        @pl.loop(0, mine)
        def _(zc):
            finish(zc)

        overlap(2)

        @pl.loop(0, mine)
        def _(zc):
            pass_on(zc)

    penalize()

    for i in range(nz):
        forward(i, drain=True)
        for n in range(slices):
            hand_over(i, n, drain=True)

    @pl.loop(0, nz)
    def _(zz):
        for u in range(1, ny):
            my_copy(zz, lax.rem(y + u, ny)).wait_send()
        for other in range(1, states):
            mx_copy(zz, y, lax.rem(k + other, states)).wait_send()

    share(drain=True)
    for send, number, _ in stages:
        for u in range(1, number):
            send(u).wait_send()

    @pl.loop(0, mine)
    def _(zc):
        for u in range(1, ny):
            t_copy(zc, lax.rem(y + u, ny)).wait_send()
        for kk in range(states):
            @pl.when(kk != k)
            def _():
                r_copy(kk, zc).wait_send()

            deliver(kk, zc, drain=True)

    for copy in pen_copies:
        copy.wait()
    if direct:
        rest = next_hbm.at[:, pl.ds(0, (bonds - ny) * w)]
    else:
        rest = next_hbm.at[pl.ds(0, bonds - ny)]
    remote(rest, rest, n_send, n_recv, k, me).wait_recv()


def shards(states, bonds, intersect_left, stored_block, stored_site, current_site, current_block, penalty_weight):
    rows, width = intersect_left.shape[1:]
    pairs, w = stored_block.shape[1:3]
    phys = stored_site.shape[1]
    fwidth = current_site.shape[2]
    groups = width // TILE
    gpp = groups // states
    ny = 1
    while 4 * ny * ny <= bonds // CORES:
        ny *= 2
    nz = bonds // (CORES * ny)
    direct = w % 128 == 0
    fch = ny * w if direct else max(w, 128)
    nch, mine = fwidth // fch, fwidth // w // ny
    cell = CORES * rows
    piece = phys * cell
    bf, f32 = jnp.bfloat16, jnp.float32
    anywhere = pl.BlockSpec(memory_space=pl.ANY)
    dma = pltpu.SemaphoreType.DMA
    penalized, grown = pl.pallas_call(
        functools.partial(kernel, states, bonds, ny, fch),
        out_shape=(
            jax.ShapeDtypeStruct(current_block.shape, f32),
            jax.ShapeDtypeStruct((w, bonds * w) if direct else (bonds, w, w), bf),
        ),
        in_specs=[anywhere] * 5 + [pl.BlockSpec(memory_space=pltpu.SMEM)],
        out_specs=(anywhere, anywhere),
        scratch_shapes=[
            pltpu.VMEM((bonds, PARTS, rows // PARTS, width), bf),
            pltpu.VMEM((nch, nz, phys, CORES, rows, fch), bf),
            pltpu.VMEM(((pairs + phys) * w, width), bf),
            pltpu.VMEM((groups, pairs, w, TILE), bf),
            pltpu.VMEM((groups, PARTS, pairs * w // PARTS, TILE), bf),
            pltpu.VMEM((states, gpp, PARTS, pairs * w // PARTS, TILE), bf),
            pltpu.VMEM((nz, ny, w, piece), bf),
            pltpu.VMEM((states, ny, w, nz * piece), bf),
            pltpu.VMEM((mine, states * ny * w, w), f32),
            pltpu.VMEM((mine, ny, states * ny * w, w), bf),
            pltpu.VMEM((mine, ny, states * ny * w, w), bf),
            pltpu.VMEM((states, mine, ny, w, w), bf),
            pltpu.VMEM((states, mine, ny, w, w), bf),
            pltpu.VMEM((gpp, pairs, w, TILE), f32),
            pltpu.VMEM((CORES * ny, states, 128), f32),
            pltpu.VMEM((nz, states, 128), f32),
            pltpu.VMEM((states, states, 128), f32),
            pltpu.VMEM((states, 8, TILE), f32),
            dma((4,)), dma((2,)),
            dma, dma((bonds, PARTS)),
            dma, dma((nch, nz, CORES)),
            dma, dma((states, nz)),
            dma, dma((nz, ny)),
            dma, dma((states,)),
            dma, dma,
            dma((3,)), dma((3,)),
            dma, dma((mine, ny)),
            dma, dma((states, mine)),
            dma, dma,
        ],
        compiler_params=pltpu.CompilerParams(
            collective_id=0, has_side_effects=True, vmem_limit_bytes=60 * 1024 * 1024
        ),
    )(
        intersect_left.reshape(PARTS, rows // PARTS, width), stored_block[0], stored_site[0],
        current_site.reshape(rows, phys * fwidth), current_block, penalty_weight,
    )
    if direct:
        return penalized, grown[None]
    return penalized, grown.transpose(1, 0, 2).reshape(1, w, bonds * w)


def solution(mesh):
    placed = (
        P("state", "bond", None),
        P("state", None, "bond", None),
        P("state", None, "bond", None),
        P("bond", None, "state"),
        P(None, "bond", "state"),
        P(),
    )
    return jax.shard_map(
        functools.partial(shards, mesh.shape["state"], mesh.shape["bond"]),
        mesh=mesh,
        in_specs=placed,
        out_specs=(P(None, "bond", "state"), P("state", "bond", None)),
        check_vma=False,
    )
```

```python
import functools

import jax
import jax.numpy as jnp
from jax import lax
from jax.experimental import pallas as pl
from jax.experimental.pallas import tpu as pltpu
from jax.sharding import PartitionSpec as P

MESH = pl.DeviceIdType.MESH
CORES = 2
TILE = 256
PARTS = 2


def both(*conds):
    return functools.reduce(jnp.logical_and, conds)


def kernel(
    states, bonds, rows_y, fch,
    env_hbm, block_hbm, site_hbm, grow_hbm, current_hbm, weight_ref,
    pen_hbm, next_hbm,
    ebuf, raw, abuf, stored, cbuf, psend, precv, mown, mbuf, acc, part, prt, nsend, nbuf, pen, iplane, iline, istate, line,
    local_sem, out_sem, e_send, e_recv, a_send, a_recv, p_send, p_recv, my_send, my_recv, mx_send, mx_recv,
    c_send, c_recv, i_send, i_recv, t_send, t_recv, r_send, r_recv, n_send, n_recv,
):
    nc, ny = CORES, rows_y
    nz = bonds // (nc * ny)
    hr, width = ebuf.shape[2:]
    rows = hr * PARTS
    pairs, w = block_hbm.shape[:2]
    phys = site_hbm.shape[0]
    fwidth = grow_hbm.shape[2]
    nch = fwidth // fch
    bpc = fch // w
    fbs = fwidth // w
    mine = fbs // ny
    cell = nc * rows
    per_group = TILE // rows
    tpp = ny * cell // TILE
    cpt = TILE // cell
    groups = width // TILE
    gpp = groups // states
    ecols = states * ny * w
    direct = w % 128 == 0
    piece = phys * cell

    k = lax.axis_index("state")
    me = lax.axis_index("bond")
    c = lax.rem(me, nc)
    y = lax.rem(lax.div(me, nc), ny)
    z = lax.div(me, nc * ny)
    near = ny * nc
    slices = PARTS * tpp

    def slot(zz, yy, cc):
        return (zz * ny + yy) * nc + cc

    sib = slot(z, y, 1 - c)

    def column_of(h, q):
        if direct:
            return (h // nc * ny + q) * nc + h % nc
        return h * bpc + q

    e_load = pltpu.make_async_copy(env_hbm, ebuf.at[me], local_sem.at[0])
    e_load.start()
    a_load = pltpu.make_async_copy(grow_hbm, raw, local_sem.at[1])
    a_load.start()
    loads = []
    for q in range(pairs):
        loads.append(pltpu.make_async_copy(block_hbm.at[q], stored.at[pl.ds(q * w, w)], local_sem.at[2]))
    for s in range(phys):
        loads.append(
            pltpu.make_async_copy(site_hbm.at[s], stored.at[pl.ds((pairs + s) * w, w)], local_sem.at[2])
        )
    for copy in loads:
        copy.start()
    c_loads = [
        pltpu.make_async_copy(
            current_hbm.at[:, :, pl.ds(g * TILE, TILE)], cbuf.at[k * gpp + g], local_sem.at[3]
        )
        for g in range(gpp)
    ]
    for copy in c_loads:
        copy.start()

    barrier = pltpu.get_barrier_semaphore()

    def greet(kk, dest):
        pl.semaphore_signal(barrier, inc=1, device_id=(kk, dest), device_id_type=MESH)

    @pl.when(z > 0)
    def _():
        greet(k, slot(z - 1, y, c))

    @pl.when(z < nz - 1)
    def _():
        greet(k, slot(z + 1, y, c))

    for other in range(1, near):
        greet(k, z * near + lax.rem(lax.rem(me, near) + other, near))
    for other in range(1, states):
        greet(lax.rem(k + other, states), me)
    ends = jnp.where(z > 0, 1, 0) + jnp.where(z < nz - 1, 1, 0)
    pl.semaphore_wait(barrier, near + states - 2 + ends)

    def remote(src, dst, ss, rs, kk, dest):
        return pltpu.make_async_remote_copy(
            src_ref=src, dst_ref=dst, send_sem=ss, recv_sem=rs, device_id=(kk, dest), device_id_type=MESH
        )

    def act(copy, drain):
        if drain:
            copy.wait_send()
        else:
            copy.start()


    def e_copy(blk, h, dest):
        ref = ebuf.at[blk, h]
        return remote(ref, ref, e_send, e_recv.at[blk, h], k, dest)

    def spread(blk, h, drain):
        @pl.when(y > 0)
        def _():
            act(e_copy(blk, h, slot(z, y - 1, c)), drain)

        @pl.when(y < ny - 1)
        def _():
            act(e_copy(blk, h, slot(z, y + 1, c)), drain)

        act(e_copy(blk, h, sib), drain)

    def column(i, drain=False):
        for h in range(PARTS):
            if i == 0:
                @pl.when(z > 0)
                def _():
                    act(e_copy(me, h, slot(z - 1, y, c)), drain)

                @pl.when(z < nz - 1)
                def _():
                    act(e_copy(me, h, slot(z + 1, y, c)), drain)

                spread(me, h, drain)
                continue
            for sign in (1, -1):
                zz = z - sign * i
                onward = z + sign

                @pl.when(both(zz >= 0, zz < nz))
                def _():
                    blk = slot(zz, y, c)
                    if not drain:
                        e_copy(blk, h, me).wait_recv()

                    @pl.when(both(onward >= 0, onward < nz))
                    def _():
                        act(e_copy(blk, h, slot(onward, y, c)), drain)

                    spread(blk, h, drain)

    def turn(j):
        least = jnp.minimum(z, nz - 1 - z)
        near = (j + 1) // 2
        inner = z - near if j % 2 else z + near
        far = j - least
        outer = jnp.where(z <= nz - 1 - z, z + far, z - far)
        return jnp.where(j <= 2 * least, inner, outer)

    def across(j, drain=False):
        zz = turn(j)
        for h in range(PARTS):
            for u in range(1, ny):
                for sign in (1, -1):
                    yy = y - sign * u
                    onward = y + sign

                    @pl.when(both(yy >= 0, yy < ny))
                    def _():
                        blk = slot(zz, yy, c)
                        if not drain:
                            e_copy(blk, h, me).wait_recv()

                        @pl.when(both(onward >= 0, onward < ny))
                        def _():
                            act(e_copy(blk, h, slot(z, onward, c)), drain)

                        act(e_copy(blk, h, sib), drain)

    def sibling(j):
        zz = turn(j)
        for h in range(PARTS):
            for yy in range(ny):
                e_copy(slot(zz, yy, 1 - c), h, me).wait_recv()


    def unpack():
        for s in range(phys):
            plain = raw[:, s, :]
            for h in range(nch):
                for q in range(bpc):
                    at = column_of(h, q) * w
                    abuf[h, z, s, c, :, q * w : (q + 1) * w] = plain[:, at : at + w]

    def a_copy(h, zz, cc, dest):
        ref = abuf.at[h, zz, :, cc]
        return remote(ref, ref, a_send, a_recv.at[h, zz, cc], k, dest)

    def a_own(sign, drain=False):
        @pl.loop(0, nch)
        def _(h):
            act(a_copy(h, z, c, slot(z + sign, y, c)), drain)

    def a_edges(i, drain=False):
        @pl.when(both(z == i, z < nz - 1))
        def _():
            a_own(1, drain)

        @pl.when(both(nz - 1 - z == i, z > 0))
        def _():
            a_own(-1, drain)

    def a_sibling(drain=False):
        @pl.loop(0, nch)
        def _(h):
            act(a_copy(h, z, c, sib), drain)

    def a_pass(h, i, drain=False):
        for sign in (1, -1):
            zz = z - sign * i
            onward = z + sign

            @pl.when(both(zz >= 0, zz < nz, onward >= 0, onward < nz))
            def _():
                if not drain:
                    a_copy(h, zz, c, me).wait_recv()
                act(a_copy(h, zz, c, slot(onward, y, c)), drain)
                act(a_copy(h, zz, c, sib), drain)

    def a_last(h, i, drain=False):
        for sign in (1, -1):
            zz = z - sign * i
            onward = z + sign

            @pl.when(both(zz >= 0, zz < nz, jnp.logical_or(onward < 0, onward >= nz)))
            def _():
                if not drain:
                    a_copy(h, zz, c, me).wait_recv()
                act(a_copy(h, zz, c, sib), drain)

    def a_ready(h):
        for zz in range(nz):
            a_copy(h, zz, 1 - c, me).wait_recv()


    def c_copy(zz, peer):
        ref = cbuf.at[pl.ds(zz * tpp, tpp)]
        return remote(ref, ref, c_send, c_recv, peer, me)

    def owner_of(zz):
        return lax.div(zz * tpp, gpp)

    def share(drain=False):
        zz = turn(nz - 1)

        @pl.when(owner_of(zz) == k)
        def _():
            for other in range(1, states):
                act(c_copy(zz, lax.rem(k + other, states)), drain)


    def p_copy(g, part_of, peer):
        return remote(
            psend.at[g, part_of], precv.at[k, lax.rem(g, gpp), part_of],
            p_send, p_recv.at[k, lax.div(g, tpp)], peer, me,
        )

    def span(zz):
        return pl.ds(pl.multiple_of(zz * piece, 128), piece)

    def my_copy(zz, yy):
        return remote(
            mown.at[zz, yy], mbuf.at[k, y, :, span(zz)], my_send, my_recv.at[zz, y], k, slot(z, yy, c)
        )

    def mx_copy(zz, yy, peer):
        ref = mbuf.at[k, yy, :, span(zz)]
        return remote(ref, ref, mx_send, mx_recv.at[k], peer, me)

    def flat_of(kk, at):
        return precv[kk, at].reshape(pairs * w, TILE).astype(jnp.float32)

    def halves(whole):
        return whole.astype(jnp.bfloat16).reshape(PARTS, pairs * w // PARTS, TILE)

    def tally(kk, g, whole):
        here = cbuf[g].reshape(pairs * w, TILE).astype(jnp.float32)
        line[kk] += jnp.sum((whole * here).reshape(pairs * w // 8, 8, TILE), axis=0)

    def p_wait(j, use):
        zz = turn(j)

        @pl.when(owner_of(zz) == k)
        def _():
            first = lax.rem(zz * tpp, gpp)
            for other in range(1, states):
                peer = lax.rem(k + other, states)
                ref = precv.at[peer, pl.ds(first, tpp)]
                remote(ref, ref, p_send, p_recv.at[peer, zz], peer, me).wait_recv()
                if use:
                    @pl.loop(0, tpp)
                    def _(r):
                        tally(peer, zz * tpp + r, flat_of(peer, first + r))

    def project(j):
        zz = turn(j)

        if j == nz - 1:
            @pl.when(owner_of(zz) != k)
            def _():
                c_copy(zz, k).wait_recv()

        @pl.loop(0, tpp)
        def _(r):
            g = zz * tpp + r
            left = ebuf[pl.ds(g * per_group, per_group)].reshape(TILE, width)
            prod = lax.dot_general(
                stored[...], left, (((1,), (1,)), ((), ())), preferred_element_type=jnp.float32
            )
            for q in range(cpt):
                yy = r * cpt + q
                moved = jnp.concatenate(
                    [
                        prod[(pairs + s) * w : (pairs + s + 1) * w, q * cell : (q + 1) * cell]
                        for s in range(phys)
                    ],
                    axis=1,
                ).astype(jnp.bfloat16)

                @pl.when(yy == y)
                def _():
                    mbuf[k, y, :, span(zz)] = moved
                    for other in range(1, states):
                        mx_copy(zz, y, lax.rem(k + other, states)).start()

                @pl.when(yy != y)
                def _():
                    mown[zz, yy] = moved
                    if j >= nz - 2:
                        my_copy(zz, yy).start()

            whole = prod[: pairs * w]
            owner = lax.div(g, gpp)

            @pl.when(jnp.logical_or(owner == k, j == nz - 1))
            def _():
                tally(k, g, whole)

            @pl.when(owner == k)
            def _():
                precv[k, lax.rem(g, gpp)] = halves(whole)

            @pl.when(owner != k)
            def _():
                psend[g] = halves(whole)

    def hand_over(j, n, drain=False):
        zz = turn(j)
        g = zz * tpp + n // PARTS
        for other in range(1, states):
            peer = lax.rem(k + other, states)

            @pl.when(lax.div(g, gpp) == peer)
            def _():
                act(p_copy(g, n % PARTS, peer), drain)

    def forward(j, drain=False):
        zz = turn(j)
        for u in range(1, ny):
            yy = lax.rem(y + u, ny)
            if not drain:
                ref = mbuf.at[k, yy, :, span(zz)]
                remote(ref, ref, my_send, my_recv.at[zz, yy], k, me).wait_recv()
            for other in range(1, states):
                act(mx_copy(zz, yy, lax.rem(k + other, states)), drain)


    def t_copy(zc, yy):
        return remote(
            part.at[zc, yy], prt.at[zc, y], t_send, t_recv.at[zc, y], k, slot(z, yy, c)
        )

    def grow(h):
        total = jnp.dot(
            mbuf[...].reshape(ecols, nz * piece),
            abuf[h].reshape(nz * piece, fch),
            preferred_element_type=jnp.float32,
        )
        for q in range(bpc):
            if direct:
                zc, yy = h, q
            else:
                fb = h * bpc + q
                zc = lax.div(fb, ny * nc) * nc + lax.rem(fb, nc)
                yy = lax.rem(lax.div(fb, nc), ny)
            block = total[:, q * w : (q + 1) * w]

            @pl.when(yy == y)
            def _():
                acc[zc] = block

            @pl.when(yy != y)
            def _():
                part[zc, yy] = block.astype(jnp.bfloat16)
                t_copy(zc, yy).start()

    def target(kk, zc):
        return slot(kk * (nz // states) + lax.div(zc, nc), y, lax.rem(zc, nc))

    def place(src):
        if direct:
            return next_hbm.at[:, pl.ds(pl.multiple_of(src * w, 128), w)]
        return next_hbm.at[src]


    def n_copy(kk, zc, yy):
        return remote(
            nbuf.at[kk, zc, yy], place(slot(z, yy, c)), n_send, n_recv, k, target(kk, zc)
        )

    def n_local(kk, zc, yy):
        return pltpu.make_async_copy(nbuf.at[kk, zc, yy], place(slot(z, yy, c)), out_sem.at[1])

    def deliver(kk, zc, drain=False):
        stays = target(kk, zc) == me
        for yy in range(ny):
            @pl.when(stays)
            def _():
                if drain:
                    n_local(kk, zc, yy).wait()
                else:
                    n_local(kk, zc, yy).start()

            @pl.when(jnp.logical_not(stays))
            def _():
                act(n_copy(kk, zc, yy), drain)

    def r_copy(kk, zc):
        return remote(nsend.at[kk, zc], nbuf.at[k, zc], r_send, r_recv.at[k, zc], kk, me)

    def finish(zc):
        total = acc[zc]
        for u in range(1, ny):
            yy = lax.rem(y + u, ny)
            ref = prt.at[zc, yy]
            remote(ref, ref, t_send, t_recv.at[zc, yy], k, me).wait_recv()
            total = total + ref[...].astype(jnp.float32)
        for kk in range(states):
            blocks = [
                total[(kk * ny + yy) * w : (kk * ny + yy + 1) * w].T.astype(jnp.bfloat16)
                for yy in range(ny)
            ]

            @pl.when(kk == k)
            def _():
                for yy in range(ny):
                    nbuf[k, zc, yy] = blocks[yy]
                deliver(k, zc)

            @pl.when(kk != k)
            def _():
                for yy in range(ny):
                    nsend[kk, zc, yy] = blocks[yy]
                r_copy(kk, zc).start()

    def pass_on(zc):
        for other in range(1, states):
            kk = lax.rem(k + other, states)
            ref = nbuf.at[kk, zc]
            remote(ref, ref, r_send, r_recv.at[kk, zc], k, me).wait_recv()
            deliver(kk, zc)


    def i_near(u):
        there = lax.rem(lax.rem(me, near) + u, near)
        ref = iplane.at[lax.rem(me, near)]
        return remote(ref, ref, i_send.at[0], i_recv.at[0], k, z * near + there)

    def i_far(u):
        ref = iline.at[z]
        return remote(ref, ref, i_send.at[1], i_recv.at[1], k, slot(lax.rem(z + u, nz), y, c))

    def i_peer(u):
        ref = istate.at[k]
        return remote(ref, ref, i_send.at[2], i_recv.at[2], lax.rem(k + u, states), me)

    stages = ((i_near, near, iplane), (i_far, nz, iline), (i_peer, states, istate))

    def start(n):
        send, number, _ = stages[n]
        for u in range(1, number):
            send(u).start()

    def gathered(n):
        _, number, buf = stages[n]
        rest = buf.at[pl.ds(0, number - 1)]
        remote(rest, rest, i_send.at[n], i_recv.at[n], k, me).wait_recv()

    def overlap(n):
        if n == 0:
            for kk in range(states):
                short = jnp.sum(line[kk], axis=0, keepdims=True)
                total = short[:, :128]
                for at in range(128, TILE, 128):
                    total = total + short[:, at : at + 128]
                iplane[lax.rem(me, near), kk : kk + 1] = total
        elif n == 1:
            gathered(0)
            iline[z] = jnp.sum(iplane[...], axis=0)
        else:
            gathered(1)
            istate[k] = jnp.sum(iline[...], axis=0)
        start(n)

    pen_copies = [
        pltpu.make_async_copy(pen.at[g], pen_hbm.at[:, :, pl.ds(g * TILE, TILE)], out_sem.at[0])
        for g in range(gpp)
    ]

    def penalize():
        gathered(2)
        p_wait(nz - 1, False)
        scale = 1.0 / (phys * width)
        factors = [weight_ref[kk] * (jnp.sum(istate[:, kk]) * scale) for kk in range(states)]
        for g in range(gpp):
            value = cbuf[k * gpp + g].reshape(pairs * w, TILE).astype(jnp.float32)
            for kk in range(states):
                value = value + factors[kk] * flat_of(kk, g)
            pen[g] = value.reshape(pairs, w, TILE)
            pen_copies[g].start()

    line[...] = jnp.zeros_like(line)
    e_load.wait()
    for i in range(nz + 1):
        if i < nz:
            column(i)
            if i == 0:
                a_load.wait()
                unpack()
                a_sibling()
            a_edges(i)
            if i == 0:
                for copy in c_loads:
                    copy.wait()
                share()
        if i == nz - 1:
            for j in range(nz - 2):
                for u in range(1, ny):
                    my_copy(turn(j), lax.rem(y + u, ny)).start()
        if i >= 1:
            across(i - 1)
            sibling(i - 1)
            if i == 1:
                for copy in loads:
                    copy.wait()
            project(i - 1)
            if i < nz:
                for n in range(slices - (i == nz - 1)):
                    hand_over(i - 1, n)
        if i == nz - 1:
            @pl.loop(0, nch)
            def _(h):
                a_pass(h, 1)

    for i in range(2, nz):
        @pl.loop(0, nch)
        def _(h):
            a_pass(h, i)

    for j in range(nz):
        forward(j)
        if 1 <= j < nz - 1:
            @pl.loop(0, nch)
            def _(h):
                a_last(h, j)
    for i in range(nz):
        column(i, drain=True)
        across(i, drain=True)
    a_last(0, nz - 1)
    for other in range(1, states):
        peer = lax.rem(k + other, states)
        ref = mbuf.at[peer]
        remote(ref, ref, mx_send, mx_recv.at[peer], peer, me).wait_recv()

    @pl.loop(0, nch)
    def _(h):
        a_ready(h)
        grow(h)

        @pl.when(h == 0)
        def _():
            hand_over(nz - 2, slices - 1)

        for n in range(slices - 1):
            @pl.when(h == min(n + 1, nch - 1))
            def _():
                hand_over(nz - 1, n)

        @pl.when(h < nch - 1)
        def _():
            a_last(h + 1, nz - 1)

        @pl.when(h == max(nch - 2, 0))
        def _():
            for j in range(nz - 1):
                p_wait(j, True)
            overlap(0)

        if direct:
            @pl.when(h > 1)
            def _():
                finish(h - 2)

    if direct:
        pass_on(0)
        overlap(1)
        finish(nch - 2)
        for h in range(1, nch - 2):
            pass_on(h)
        finish(nch - 1)
        hand_over(nz - 1, slices - 1)
        overlap(2)
        for h in range(max(nch - 2, 1), nch):
            pass_on(h)
    else:
        hand_over(nz - 1, slices - 1)
        overlap(1)

        @pl.loop(0, mine)
        def _(zc):
            finish(zc)

        overlap(2)

        @pl.loop(0, mine)
        def _(zc):
            pass_on(zc)

    penalize()
    for i in range(nz):
        a_edges(i, drain=True)
    a_sibling(drain=True)

    @pl.loop(0, nch)
    def _(h):
        for i in range(1, nz):
            a_pass(h, i, drain=True)
            a_last(h, i, drain=True)

    for i in range(nz):
        forward(i, drain=True)
        for n in range(slices):
            hand_over(i, n, drain=True)

    @pl.loop(0, nz)
    def _(zz):
        for u in range(1, ny):
            my_copy(zz, lax.rem(y + u, ny)).wait_send()
        for other in range(1, states):
            mx_copy(zz, y, lax.rem(k + other, states)).wait_send()

    share(drain=True)
    for send, number, _ in stages:
        for u in range(1, number):
            send(u).wait_send()

    @pl.loop(0, mine)
    def _(zc):
        for u in range(1, ny):
            t_copy(zc, lax.rem(y + u, ny)).wait_send()
        for kk in range(states):
            @pl.when(kk != k)
            def _():
                r_copy(kk, zc).wait_send()

            deliver(kk, zc, drain=True)

    for copy in pen_copies:
        copy.wait()
    if direct:
        rest = next_hbm.at[:, pl.ds(0, (bonds - ny) * w)]
    else:
        rest = next_hbm.at[pl.ds(0, bonds - ny)]
    remote(rest, rest, n_send, n_recv, k, me).wait_recv()


def shards(states, bonds, intersect_left, stored_block, stored_site, current_site, current_block, penalty_weight):
    rows, width = intersect_left.shape[1:]
    pairs, w = stored_block.shape[1:3]
    phys = stored_site.shape[1]
    fwidth = current_site.shape[2]
    groups = width // TILE
    gpp = groups // states
    ny = 1
    while 4 * ny * ny <= bonds // CORES:
        ny *= 2
    nz = bonds // (CORES * ny)
    direct = w % 128 == 0
    fch = ny * w if direct else max(w, 128)
    nch, mine = fwidth // fch, fwidth // w // ny
    cell = CORES * rows
    piece = phys * cell
    bf, f32 = jnp.bfloat16, jnp.float32
    anywhere = pl.BlockSpec(memory_space=pl.ANY)
    dma = pltpu.SemaphoreType.DMA
    penalized, grown = pl.pallas_call(
        functools.partial(kernel, states, bonds, ny, fch),
        out_shape=(
            jax.ShapeDtypeStruct(current_block.shape, f32),
            jax.ShapeDtypeStruct((w, bonds * w) if direct else (bonds, w, w), bf),
        ),
        in_specs=[anywhere] * 5 + [pl.BlockSpec(memory_space=pltpu.SMEM)],
        out_specs=(anywhere, anywhere),
        scratch_shapes=[
            pltpu.VMEM((bonds, PARTS, rows // PARTS, width), bf),
            pltpu.VMEM((rows, phys, fwidth), bf),
            pltpu.VMEM((nch, nz, phys, CORES, rows, fch), bf),
            pltpu.VMEM(((pairs + phys) * w, width), bf),
            pltpu.VMEM((groups, pairs, w, TILE), bf),
            pltpu.VMEM((groups, PARTS, pairs * w // PARTS, TILE), bf),
            pltpu.VMEM((states, gpp, PARTS, pairs * w // PARTS, TILE), bf),
            pltpu.VMEM((nz, ny, w, piece), bf),
            pltpu.VMEM((states, ny, w, nz * piece), bf),
            pltpu.VMEM((mine, states * ny * w, w), f32),
            pltpu.VMEM((mine, ny, states * ny * w, w), bf),
            pltpu.VMEM((mine, ny, states * ny * w, w), bf),
            pltpu.VMEM((states, mine, ny, w, w), bf),
            pltpu.VMEM((states, mine, ny, w, w), bf),
            pltpu.VMEM((gpp, pairs, w, TILE), f32),
            pltpu.VMEM((CORES * ny, states, 128), f32),
            pltpu.VMEM((nz, states, 128), f32),
            pltpu.VMEM((states, states, 128), f32),
            pltpu.VMEM((states, 8, TILE), f32),
            dma((4,)), dma((2,)),
            dma, dma((bonds, PARTS)),
            dma, dma((nch, nz, CORES)),
            dma, dma((states, nz)),
            dma, dma((nz, ny)),
            dma, dma((states,)),
            dma, dma,
            dma((3,)), dma((3,)),
            dma, dma((mine, ny)),
            dma, dma((states, mine)),
            dma, dma,
        ],
        compiler_params=pltpu.CompilerParams(
            collective_id=0, has_side_effects=True, vmem_limit_bytes=60 * 1024 * 1024
        ),
    )(
        intersect_left.reshape(PARTS, rows // PARTS, width), stored_block[0], stored_site[0],
        current_site, current_block, penalty_weight,
    )
    if direct:
        return penalized, grown[None]
    return penalized, grown.transpose(1, 0, 2).reshape(1, w, bonds * w)


def solution(mesh):
    placed = (
        P("state", "bond", None),
        P("state", None, "bond", None),
        P("state", None, "bond", None),
        P("bond", None, "state"),
        P(None, "bond", "state"),
        P(),
    )
    return jax.shard_map(
        functools.partial(shards, mesh.shape["state"], mesh.shape["bond"]),
        mesh=mesh,
        in_specs=placed,
        out_specs=(P(None, "bond", "state"), P("state", "bond", None)),
        check_vma=False,
    )
```

```python
import functools

import jax
import jax.numpy as jnp
from jax import lax
from jax.experimental import pallas as pl
from jax.experimental.pallas import tpu as pltpu
from jax.sharding import PartitionSpec as P

MESH = pl.DeviceIdType.MESH
CORES = 2
TILE = 256
PARTS = 2


def both(*conds):
    return functools.reduce(jnp.logical_and, conds)


def kernel(
    states, bonds, rows_y, fch,
    env_hbm, block_hbm, site_hbm, grow_hbm, current_hbm, weight_ref,
    pen_ref, next_ref,
    ebuf, raw, abuf, stored, cbuf, psend, precv, mown, mbuf, acc, part, prt, nsend, nbuf, iplane, iline, istate, line,
    local_sem, e_send, e_recv, a_send, a_recv, p_send, p_recv, my_send, my_recv, mx_send, mx_recv,
    c_send, c_recv, i_send, i_recv, t_send, t_recv, r_send, r_recv, n_send, n_recv,
):
    nc, ny = CORES, rows_y
    nz = bonds // (nc * ny)
    hr, width = ebuf.shape[2:]
    rows = hr * PARTS
    pairs, w = block_hbm.shape[:2]
    phys = site_hbm.shape[0]
    fwidth = grow_hbm.shape[2]
    nch = fwidth // fch
    bpc = fch // w
    fbs = fwidth // w
    mine = fbs // ny
    cell = nc * rows
    per_group = TILE // rows
    tpp = ny * cell // TILE
    cpt = TILE // cell
    groups = width // TILE
    gpp = groups // states
    ecols = states * ny * w
    direct = w % 128 == 0
    piece = phys * cell

    k = lax.axis_index("state")
    me = lax.axis_index("bond")
    c = lax.rem(me, nc)
    y = lax.rem(lax.div(me, nc), ny)
    z = lax.div(me, nc * ny)
    near = ny * nc
    slices = PARTS * tpp

    def slot(zz, yy, cc):
        return (zz * ny + yy) * nc + cc

    sib = slot(z, y, 1 - c)

    def column_of(h, q):
        if direct:
            return (h // nc * ny + q) * nc + h % nc
        return h * bpc + q

    e_load = pltpu.make_async_copy(env_hbm, ebuf.at[me], local_sem.at[0])
    e_load.start()
    a_load = pltpu.make_async_copy(grow_hbm, raw, local_sem.at[1])
    a_load.start()
    loads = []
    for q in range(pairs):
        loads.append(pltpu.make_async_copy(block_hbm.at[q], stored.at[pl.ds(q * w, w)], local_sem.at[2]))
    for s in range(phys):
        loads.append(
            pltpu.make_async_copy(site_hbm.at[s], stored.at[pl.ds((pairs + s) * w, w)], local_sem.at[2])
        )
    for copy in loads:
        copy.start()
    c_loads = [
        pltpu.make_async_copy(
            current_hbm.at[:, :, pl.ds(g * TILE, TILE)], cbuf.at[k * gpp + g], local_sem.at[3]
        )
        for g in range(gpp)
    ]
    for copy in c_loads:
        copy.start()

    barrier = pltpu.get_barrier_semaphore()

    def greet(kk, dest):
        pl.semaphore_signal(barrier, inc=1, device_id=(kk, dest), device_id_type=MESH)

    @pl.when(z > 0)
    def _():
        greet(k, slot(z - 1, y, c))

    @pl.when(z < nz - 1)
    def _():
        greet(k, slot(z + 1, y, c))

    for other in range(1, near):
        greet(k, z * near + lax.rem(lax.rem(me, near) + other, near))
    for other in range(1, states):
        greet(lax.rem(k + other, states), me)
    ends = jnp.where(z > 0, 1, 0) + jnp.where(z < nz - 1, 1, 0)
    pl.semaphore_wait(barrier, near + states - 2 + ends)

    def remote(src, dst, ss, rs, kk, dest):
        return pltpu.make_async_remote_copy(
            src_ref=src, dst_ref=dst, send_sem=ss, recv_sem=rs, device_id=(kk, dest), device_id_type=MESH
        )

    def act(copy, drain):
        if drain:
            copy.wait_send()
        else:
            copy.start()


    def e_copy(blk, h, dest):
        ref = ebuf.at[blk, h]
        return remote(ref, ref, e_send, e_recv.at[blk, h], k, dest)

    def spread(blk, h, drain):
        @pl.when(y > 0)
        def _():
            act(e_copy(blk, h, slot(z, y - 1, c)), drain)

        @pl.when(y < ny - 1)
        def _():
            act(e_copy(blk, h, slot(z, y + 1, c)), drain)

        act(e_copy(blk, h, sib), drain)

    def column(i, drain=False):
        for h in range(PARTS):
            if i == 0:
                @pl.when(z > 0)
                def _():
                    act(e_copy(me, h, slot(z - 1, y, c)), drain)

                @pl.when(z < nz - 1)
                def _():
                    act(e_copy(me, h, slot(z + 1, y, c)), drain)

                spread(me, h, drain)
                continue
            for sign in (1, -1):
                zz = z - sign * i
                onward = z + sign

                @pl.when(both(zz >= 0, zz < nz))
                def _():
                    blk = slot(zz, y, c)
                    if not drain:
                        e_copy(blk, h, me).wait_recv()

                    @pl.when(both(onward >= 0, onward < nz))
                    def _():
                        act(e_copy(blk, h, slot(onward, y, c)), drain)

                    spread(blk, h, drain)

    def turn(j):
        least = jnp.minimum(z, nz - 1 - z)
        near = (j + 1) // 2
        inner = z - near if j % 2 else z + near
        far = j - least
        outer = jnp.where(z <= nz - 1 - z, z + far, z - far)
        return jnp.where(j <= 2 * least, inner, outer)

    def across(j, drain=False):
        zz = turn(j)
        for h in range(PARTS):
            for u in range(1, ny):
                for sign in (1, -1):
                    yy = y - sign * u
                    onward = y + sign

                    @pl.when(both(yy >= 0, yy < ny))
                    def _():
                        blk = slot(zz, yy, c)
                        if not drain:
                            e_copy(blk, h, me).wait_recv()

                        @pl.when(both(onward >= 0, onward < ny))
                        def _():
                            act(e_copy(blk, h, slot(z, onward, c)), drain)

                        act(e_copy(blk, h, sib), drain)

    def sibling(j):
        zz = turn(j)
        for h in range(PARTS):
            for yy in range(ny):
                e_copy(slot(zz, yy, 1 - c), h, me).wait_recv()


    def unpack():
        for s in range(phys):
            plain = raw[:, s, :]
            for h in range(nch):
                for q in range(bpc):
                    at = column_of(h, q) * w
                    abuf[h, z, s, c, :, q * w : (q + 1) * w] = plain[:, at : at + w]

    def a_copy(h, zz, cc, dest):
        ref = abuf.at[h, zz, :, cc]
        return remote(ref, ref, a_send, a_recv.at[h, zz, cc], k, dest)

    def a_own(sign, drain=False):
        @pl.loop(0, nch)
        def _(h):
            act(a_copy(h, z, c, slot(z + sign, y, c)), drain)

    def a_edges(i, drain=False):
        @pl.when(both(z == i, z < nz - 1))
        def _():
            a_own(1, drain)

        @pl.when(both(nz - 1 - z == i, z > 0))
        def _():
            a_own(-1, drain)

    def a_sibling(drain=False):
        @pl.loop(0, nch)
        def _(h):
            act(a_copy(h, z, c, sib), drain)

    def a_pass(h, i, drain=False):
        for sign in (1, -1):
            zz = z - sign * i
            onward = z + sign

            @pl.when(both(zz >= 0, zz < nz, onward >= 0, onward < nz))
            def _():
                if not drain:
                    a_copy(h, zz, c, me).wait_recv()
                act(a_copy(h, zz, c, slot(onward, y, c)), drain)
                act(a_copy(h, zz, c, sib), drain)

    def a_last(h, i, drain=False):
        for sign in (1, -1):
            zz = z - sign * i
            onward = z + sign

            @pl.when(both(zz >= 0, zz < nz, jnp.logical_or(onward < 0, onward >= nz)))
            def _():
                if not drain:
                    a_copy(h, zz, c, me).wait_recv()
                act(a_copy(h, zz, c, sib), drain)

    def a_ready(h):
        for zz in range(nz):
            a_copy(h, zz, 1 - c, me).wait_recv()


    def c_copy(zz, peer):
        ref = cbuf.at[pl.ds(zz * tpp, tpp)]
        return remote(ref, ref, c_send, c_recv, peer, me)

    def owner_of(zz):
        return lax.div(zz * tpp, gpp)

    def share(drain=False):
        zz = turn(nz - 1)

        @pl.when(owner_of(zz) == k)
        def _():
            for other in range(1, states):
                act(c_copy(zz, lax.rem(k + other, states)), drain)


    def p_copy(g, part_of, peer):
        return remote(
            psend.at[g, part_of], precv.at[k, lax.rem(g, gpp), part_of],
            p_send, p_recv.at[k, lax.div(g, tpp)], peer, me,
        )

    def span(zz):
        return pl.ds(pl.multiple_of(zz * piece, 128), piece)

    def my_copy(zz, yy):
        return remote(
            mown.at[zz, yy], mbuf.at[k, y, :, span(zz)], my_send, my_recv.at[zz, y], k, slot(z, yy, c)
        )

    def mx_copy(zz, yy, peer):
        ref = mbuf.at[k, yy, :, span(zz)]
        return remote(ref, ref, mx_send, mx_recv.at[k], peer, me)

    def flat_of(kk, at):
        return precv[kk, at].reshape(pairs * w, TILE).astype(jnp.float32)

    def halves(whole):
        return whole.astype(jnp.bfloat16).reshape(PARTS, pairs * w // PARTS, TILE)

    def tally(kk, g, whole):
        here = cbuf[g].reshape(pairs * w, TILE).astype(jnp.float32)
        line[kk] += jnp.sum((whole * here).reshape(pairs * w // 8, 8, TILE), axis=0)

    def p_wait(j, use):
        zz = turn(j)

        @pl.when(owner_of(zz) == k)
        def _():
            first = lax.rem(zz * tpp, gpp)
            for other in range(1, states):
                peer = lax.rem(k + other, states)
                ref = precv.at[peer, pl.ds(first, tpp)]
                remote(ref, ref, p_send, p_recv.at[peer, zz], peer, me).wait_recv()
                if use:
                    @pl.loop(0, tpp)
                    def _(r):
                        tally(peer, zz * tpp + r, flat_of(peer, first + r))

    def project(j):
        zz = turn(j)

        if j == nz - 1:
            @pl.when(owner_of(zz) != k)
            def _():
                c_copy(zz, k).wait_recv()

        @pl.loop(0, tpp)
        def _(r):
            g = zz * tpp + r
            left = ebuf[pl.ds(g * per_group, per_group)].reshape(TILE, width)
            prod = lax.dot_general(
                stored[...], left, (((1,), (1,)), ((), ())), preferred_element_type=jnp.float32
            )
            for q in range(cpt):
                yy = r * cpt + q
                moved = jnp.concatenate(
                    [
                        prod[(pairs + s) * w : (pairs + s + 1) * w, q * cell : (q + 1) * cell]
                        for s in range(phys)
                    ],
                    axis=1,
                ).astype(jnp.bfloat16)

                @pl.when(yy == y)
                def _():
                    mbuf[k, y, :, span(zz)] = moved
                    for other in range(1, states):
                        mx_copy(zz, y, lax.rem(k + other, states)).start()

                @pl.when(yy != y)
                def _():
                    mown[zz, yy] = moved
                    if j >= nz - 2:
                        my_copy(zz, yy).start()

            whole = prod[: pairs * w]
            owner = lax.div(g, gpp)

            @pl.when(jnp.logical_or(owner == k, j == nz - 1))
            def _():
                tally(k, g, whole)

            @pl.when(owner == k)
            def _():
                precv[k, lax.rem(g, gpp)] = halves(whole)

            @pl.when(owner != k)
            def _():
                psend[g] = halves(whole)

    def hand_over(j, n, drain=False):
        zz = turn(j)
        g = zz * tpp + n // PARTS
        for other in range(1, states):
            peer = lax.rem(k + other, states)

            @pl.when(lax.div(g, gpp) == peer)
            def _():
                act(p_copy(g, n % PARTS, peer), drain)

    def forward(j, drain=False):
        zz = turn(j)
        for u in range(1, ny):
            yy = lax.rem(y + u, ny)
            if not drain:
                ref = mbuf.at[k, yy, :, span(zz)]
                remote(ref, ref, my_send, my_recv.at[zz, yy], k, me).wait_recv()
            for other in range(1, states):
                act(mx_copy(zz, yy, lax.rem(k + other, states)), drain)


    def t_copy(zc, yy):
        return remote(
            part.at[zc, yy], prt.at[zc, y], t_send, t_recv.at[zc, y], k, slot(z, yy, c)
        )

    def grow(h):
        total = jnp.dot(
            mbuf[...].reshape(ecols, nz * piece),
            abuf[h].reshape(nz * piece, fch),
            preferred_element_type=jnp.float32,
        )
        for q in range(bpc):
            if direct:
                zc, yy = h, q
            else:
                fb = h * bpc + q
                zc = lax.div(fb, ny * nc) * nc + lax.rem(fb, nc)
                yy = lax.rem(lax.div(fb, nc), ny)
            block = total[:, q * w : (q + 1) * w]

            @pl.when(yy == y)
            def _():
                acc[zc] = block

            @pl.when(yy != y)
            def _():
                part[zc, yy] = block.astype(jnp.bfloat16)
                t_copy(zc, yy).start()

    def target(kk, zc):
        return slot(kk * (nz // states) + lax.div(zc, nc), y, lax.rem(zc, nc))

    def place(src):
        if direct:
            return next_ref.at[:, pl.ds(pl.multiple_of(src * w, 128), w)]
        return next_ref.at[src]


    def n_copy(kk, zc, yy):
        return remote(
            nbuf.at[kk, zc, yy], place(slot(z, yy, c)), n_send, n_recv, k, target(kk, zc)
        )

    def deliver(kk, zc, drain=False):
        stays = target(kk, zc) == me
        for yy in range(ny):
            if not drain:
                @pl.when(stays)
                def _():
                    place(slot(z, yy, c))[...] = nbuf[kk, zc, yy]

            @pl.when(jnp.logical_not(stays))
            def _():
                act(n_copy(kk, zc, yy), drain)

    def r_copy(kk, zc):
        return remote(nsend.at[kk, zc], nbuf.at[k, zc], r_send, r_recv.at[k, zc], kk, me)

    def finish(zc):
        total = acc[zc]
        for u in range(1, ny):
            yy = lax.rem(y + u, ny)
            ref = prt.at[zc, yy]
            remote(ref, ref, t_send, t_recv.at[zc, yy], k, me).wait_recv()
            total = total + ref[...].astype(jnp.float32)
        for kk in range(states):
            blocks = [
                total[(kk * ny + yy) * w : (kk * ny + yy + 1) * w].T.astype(jnp.bfloat16)
                for yy in range(ny)
            ]

            @pl.when(kk == k)
            def _():
                for yy in range(ny):
                    nbuf[k, zc, yy] = blocks[yy]
                deliver(k, zc)

            @pl.when(kk != k)
            def _():
                for yy in range(ny):
                    nsend[kk, zc, yy] = blocks[yy]
                r_copy(kk, zc).start()

    def pass_on(zc):
        for other in range(1, states):
            kk = lax.rem(k + other, states)
            ref = nbuf.at[kk, zc]
            remote(ref, ref, r_send, r_recv.at[kk, zc], k, me).wait_recv()
            deliver(kk, zc)


    def i_near(u):
        there = lax.rem(lax.rem(me, near) + u, near)
        ref = iplane.at[lax.rem(me, near)]
        return remote(ref, ref, i_send.at[0], i_recv.at[0], k, z * near + there)

    def i_far(u):
        ref = iline.at[z]
        return remote(ref, ref, i_send.at[1], i_recv.at[1], k, slot(lax.rem(z + u, nz), y, c))

    def i_peer(u):
        ref = istate.at[k]
        return remote(ref, ref, i_send.at[2], i_recv.at[2], lax.rem(k + u, states), me)

    stages = ((i_near, near, iplane), (i_far, nz, iline), (i_peer, states, istate))

    def start(n):
        send, number, _ = stages[n]
        for u in range(1, number):
            send(u).start()

    def gathered(n):
        _, number, buf = stages[n]
        rest = buf.at[pl.ds(0, number - 1)]
        remote(rest, rest, i_send.at[n], i_recv.at[n], k, me).wait_recv()

    def overlap(n):
        if n == 0:
            for kk in range(states):
                short = jnp.sum(line[kk], axis=0, keepdims=True)
                total = short[:, :128]
                for at in range(128, TILE, 128):
                    total = total + short[:, at : at + 128]
                iplane[lax.rem(me, near), kk : kk + 1] = total
        elif n == 1:
            gathered(0)
            iline[z] = jnp.sum(iplane[...], axis=0)
        else:
            gathered(1)
            istate[k] = jnp.sum(iline[...], axis=0)
        start(n)

    def penalize():
        gathered(2)
        p_wait(nz - 1, False)
        scale = 1.0 / (phys * width)
        factors = [weight_ref[kk] * (jnp.sum(istate[:, kk]) * scale) for kk in range(states)]
        for g in range(gpp):
            value = cbuf[k * gpp + g].reshape(pairs * w, TILE).astype(jnp.float32)
            for kk in range(states):
                value = value + factors[kk] * flat_of(kk, g)
            pen_ref[:, :, g * TILE : (g + 1) * TILE] = value.reshape(pairs, w, TILE)

    line[...] = jnp.zeros_like(line)
    e_load.wait()
    for i in range(nz + 1):
        if i < nz:
            column(i)
            if i == 0:
                a_load.wait()
                unpack()
                a_sibling()
            a_edges(i)
            if i == 0:
                for copy in c_loads:
                    copy.wait()
                share()
        if i == nz - 1:
            for j in range(nz - 2):
                for u in range(1, ny):
                    my_copy(turn(j), lax.rem(y + u, ny)).start()
        if i >= 1:
            across(i - 1)
            sibling(i - 1)
            if i == 1:
                for copy in loads:
                    copy.wait()
            project(i - 1)
            if i < nz:
                for n in range(slices - (i == nz - 1)):
                    hand_over(i - 1, n)
        if i == nz - 1:
            @pl.loop(0, nch)
            def _(h):
                a_pass(h, 1)

    for i in range(2, nz):
        @pl.loop(0, nch)
        def _(h):
            a_pass(h, i)

    for j in range(nz):
        forward(j)
        if 1 <= j < nz - 1:
            @pl.loop(0, nch)
            def _(h):
                a_last(h, j)
    for i in range(nz):
        column(i, drain=True)
        across(i, drain=True)
    a_last(0, nz - 1)
    for other in range(1, states):
        peer = lax.rem(k + other, states)
        ref = mbuf.at[peer]
        remote(ref, ref, mx_send, mx_recv.at[peer], peer, me).wait_recv()

    @pl.loop(0, nch)
    def _(h):
        a_ready(h)
        grow(h)

        @pl.when(h == 0)
        def _():
            hand_over(nz - 2, slices - 1)

        for n in range(slices - 1):
            @pl.when(h == min(n + 1, nch - 1))
            def _():
                hand_over(nz - 1, n)

        @pl.when(h < nch - 1)
        def _():
            a_last(h + 1, nz - 1)

        @pl.when(h == max(nch - 2, 0))
        def _():
            for j in range(nz - 1):
                p_wait(j, True)
            overlap(0)

        if direct:
            @pl.when(h > 1)
            def _():
                finish(h - 2)

    if direct:
        pass_on(0)
        overlap(1)
        finish(nch - 2)
        for h in range(1, nch - 2):
            pass_on(h)
        finish(nch - 1)
        hand_over(nz - 1, slices - 1)
        overlap(2)
        for h in range(max(nch - 2, 1), nch):
            pass_on(h)
    else:
        hand_over(nz - 1, slices - 1)
        overlap(1)

        @pl.loop(0, mine)
        def _(zc):
            finish(zc)

        overlap(2)

        @pl.loop(0, mine)
        def _(zc):
            pass_on(zc)

    penalize()
    for i in range(nz):
        a_edges(i, drain=True)
    a_sibling(drain=True)

    @pl.loop(0, nch)
    def _(h):
        for i in range(1, nz):
            a_pass(h, i, drain=True)
            a_last(h, i, drain=True)

    for i in range(nz):
        forward(i, drain=True)
        for n in range(slices):
            hand_over(i, n, drain=True)

    @pl.loop(0, nz)
    def _(zz):
        for u in range(1, ny):
            my_copy(zz, lax.rem(y + u, ny)).wait_send()
        for other in range(1, states):
            mx_copy(zz, y, lax.rem(k + other, states)).wait_send()

    share(drain=True)
    for send, number, _ in stages:
        for u in range(1, number):
            send(u).wait_send()

    @pl.loop(0, mine)
    def _(zc):
        for u in range(1, ny):
            t_copy(zc, lax.rem(y + u, ny)).wait_send()
        for kk in range(states):
            @pl.when(kk != k)
            def _():
                r_copy(kk, zc).wait_send()

            deliver(kk, zc, drain=True)

    if direct:
        rest = next_ref.at[:, pl.ds(0, (bonds - ny) * w)]
    else:
        rest = next_ref.at[pl.ds(0, bonds - ny)]
    remote(rest, rest, n_send, n_recv, k, me).wait_recv()


def shards(states, bonds, intersect_left, stored_block, stored_site, current_site, current_block, penalty_weight):
    rows, width = intersect_left.shape[1:]
    pairs, w = stored_block.shape[1:3]
    phys = stored_site.shape[1]
    fwidth = current_site.shape[2]
    groups = width // TILE
    gpp = groups // states
    ny = 1
    while 4 * ny * ny <= bonds // CORES:
        ny *= 2
    nz = bonds // (CORES * ny)
    direct = w % 128 == 0
    fch = ny * w if direct else max(w, 128)
    nch, mine = fwidth // fch, fwidth // w // ny
    cell = CORES * rows
    piece = phys * cell
    bf, f32 = jnp.bfloat16, jnp.float32
    anywhere = pl.BlockSpec(memory_space=pltpu.HBM)
    dma = pltpu.SemaphoreType.DMA
    penalized, grown = pl.pallas_call(
        functools.partial(kernel, states, bonds, ny, fch),
        out_shape=(
            pltpu.VMEM(current_block.shape, f32),
            pltpu.VMEM((w, bonds * w) if direct else (bonds, w, w), bf),
        ),
        in_specs=[anywhere] * 5 + [pl.BlockSpec(memory_space=pltpu.SMEM)],
        out_specs=(pl.BlockSpec(memory_space=pltpu.VMEM),) * 2,
        scratch_shapes=[
            pltpu.VMEM((bonds, PARTS, rows // PARTS, width), bf),
            pltpu.VMEM((rows, phys, fwidth), bf),
            pltpu.VMEM((nch, nz, phys, CORES, rows, fch), bf),
            pltpu.VMEM(((pairs + phys) * w, width), bf),
            pltpu.VMEM((groups, pairs, w, TILE), bf),
            pltpu.VMEM((groups, PARTS, pairs * w // PARTS, TILE), bf),
            pltpu.VMEM((states, gpp, PARTS, pairs * w // PARTS, TILE), bf),
            pltpu.VMEM((nz, ny, w, piece), bf),
            pltpu.VMEM((states, ny, w, nz * piece), bf),
            pltpu.VMEM((mine, states * ny * w, w), f32),
            pltpu.VMEM((mine, ny, states * ny * w, w), bf),
            pltpu.VMEM((mine, ny, states * ny * w, w), bf),
            pltpu.VMEM((states, mine, ny, w, w), bf),
            pltpu.VMEM((states, mine, ny, w, w), bf),
            pltpu.VMEM((CORES * ny, states, 128), f32),
            pltpu.VMEM((nz, states, 128), f32),
            pltpu.VMEM((states, states, 128), f32),
            pltpu.VMEM((states, 8, TILE), f32),
            dma((4,)),
            dma, dma((bonds, PARTS)),
            dma, dma((nch, nz, CORES)),
            dma, dma((states, nz)),
            dma, dma((nz, ny)),
            dma, dma((states,)),
            dma, dma,
            dma((3,)), dma((3,)),
            dma, dma((mine, ny)),
            dma, dma((states, mine)),
            dma, dma,
        ],
        compiler_params=pltpu.CompilerParams(
            collective_id=0, has_side_effects=True, vmem_limit_bytes=60 * 1024 * 1024
        ),
    )(
        intersect_left.reshape(PARTS, rows // PARTS, width), stored_block[0], stored_site[0],
        current_site, current_block, penalty_weight,
    )
    if direct:
        return penalized, grown[None]
    return penalized, grown.transpose(1, 0, 2).reshape(1, w, bonds * w)


def solution(mesh):
    placed = (
        P("state", "bond", None),
        P("state", None, "bond", None),
        P("state", None, "bond", None),
        P("bond", None, "state"),
        P(None, "bond", "state"),
        P(),
    )
    return jax.shard_map(
        functools.partial(shards, mesh.shape["state"], mesh.shape["bond"]),
        mesh=mesh,
        in_specs=placed,
        out_specs=(P(None, "bond", "state"), P("state", "bond", None)),
        check_vma=False,
    )
```

```python
import functools

import jax
import jax.numpy as jnp
from jax import lax
from jax.experimental import pallas as pl
from jax.experimental.pallas import tpu as pltpu
from jax.sharding import PartitionSpec as P

MESH = pl.DeviceIdType.MESH
CORES = 2
TILE = 256
PARTS = 2


def both(*conds):
    return functools.reduce(jnp.logical_and, conds)


def kernel(
    states, bonds, rows_y, fch,
    env_hbm, block_hbm, site_hbm, grow_hbm, current_hbm, weight_ref,
    pen_ref, next_ref,
    ebuf, raw, abuf, stored, cbuf, psend, precv, mown, mbuf, acc, part, prt, nsend, nbuf, iplane, iline, istate, line,
    local_sem, e_send, e_recv, a_send, a_recv, p_send, p_recv, my_send, my_recv, mx_send, mx_recv,
    c_send, c_recv, i_send, i_recv, t_send, t_recv, r_send, r_recv, n_send, n_recv,
):
    nc, ny = CORES, rows_y
    nz = bonds // (nc * ny)
    hr, width = ebuf.shape[2:]
    rows = hr * PARTS
    pairs, w = block_hbm.shape[:2]
    phys = site_hbm.shape[0]
    fwidth = grow_hbm.shape[2]
    nch = fwidth // fch
    bpc = fch // w
    fbs = fwidth // w
    mine = fbs // ny
    cell = nc * rows
    per_group = TILE // rows
    tpp = ny * cell // TILE
    cpt = TILE // cell
    groups = width // TILE
    gpp = groups // states
    ecols = states * ny * w
    direct = w % 128 == 0
    piece = phys * cell

    k = lax.axis_index("state")
    me = lax.axis_index("bond")
    c = lax.rem(me, nc)
    y = lax.rem(lax.div(me, nc), ny)
    z = lax.div(me, nc * ny)
    near = ny * nc
    slices = PARTS * tpp

    def slot(zz, yy, cc):
        return (zz * ny + yy) * nc + cc

    sib = slot(z, y, 1 - c)

    def owner_of(zz):
        return lax.div(zz * tpp, gpp)

    def order(kk, zz):
        rest = sorted(set(range(nz)) - {zz}, key=lambda other: abs(other - zz))
        return [zz] + sorted(rest, key=lambda other: other * tpp // gpp == kk)

    def turn_of(kk, j):
        at = jnp.int32(0)
        for k_ in range(states):
            for z_ in range(nz):
                at = at + jnp.where(both(kk == k_, z == z_), order(k_, z_)[j], 0)
        return at

    turns = [turn_of(k, j) for j in range(nz)]

    def turn(j):
        return turns[j]

    def column_of(h, q):
        if direct:
            return (h // nc * ny + q) * nc + h % nc
        return h * bpc + q

    e_load = pltpu.make_async_copy(env_hbm, ebuf.at[me], local_sem.at[0])
    e_load.start()
    a_load = pltpu.make_async_copy(grow_hbm, raw, local_sem.at[1])
    a_load.start()
    loads = []
    for q in range(pairs):
        loads.append(pltpu.make_async_copy(block_hbm.at[q], stored.at[pl.ds(q * w, w)], local_sem.at[2]))
    for s in range(phys):
        loads.append(
            pltpu.make_async_copy(site_hbm.at[s], stored.at[pl.ds((pairs + s) * w, w)], local_sem.at[2])
        )
    for copy in loads:
        copy.start()
    c_loads = [
        pltpu.make_async_copy(
            current_hbm.at[:, :, pl.ds(g * TILE, TILE)], cbuf.at[k * gpp + g], local_sem.at[3]
        )
        for g in range(gpp)
    ]
    for copy in c_loads:
        copy.start()

    barrier = pltpu.get_barrier_semaphore()

    def greet(kk, dest):
        pl.semaphore_signal(barrier, inc=1, device_id=(kk, dest), device_id_type=MESH)

    @pl.when(z > 0)
    def _():
        greet(k, slot(z - 1, y, c))

    @pl.when(z < nz - 1)
    def _():
        greet(k, slot(z + 1, y, c))

    for other in range(1, near):
        greet(k, z * near + lax.rem(lax.rem(me, near) + other, near))
    for other in range(1, states):
        greet(lax.rem(k + other, states), me)
    ends = jnp.where(z > 0, 1, 0) + jnp.where(z < nz - 1, 1, 0)
    pl.semaphore_wait(barrier, near + states - 2 + ends)

    def remote(src, dst, ss, rs, kk, dest):
        return pltpu.make_async_remote_copy(
            src_ref=src, dst_ref=dst, send_sem=ss, recv_sem=rs, device_id=(kk, dest), device_id_type=MESH
        )

    def act(copy, drain):
        if drain:
            copy.wait_send()
        else:
            copy.start()


    def e_copy(blk, h, dest):
        ref = ebuf.at[blk, h]
        return remote(ref, ref, e_send, e_recv.at[blk, h], k, dest)

    def spread(blk, h, drain=False):
        @pl.when(y > 0)
        def _():
            act(e_copy(blk, h, slot(z, y - 1, c)), drain)

        @pl.when(y < ny - 1)
        def _():
            act(e_copy(blk, h, slot(z, y + 1, c)), drain)

    def within(zz):
        return both(zz >= 0, zz < nz)


    def late(zz, sign):
        return both(owner_of(zz) == k, k != (0 if sign > 0 else states - 1))

    def pass_z(zz, h, sign, drain=False):
        @pl.when(within(z + sign))
        def _():
            act(e_copy(slot(zz, y, c), h, slot(z + sign, y, c)), drain)

    def own():
        for h in range(PARTS):
            for sign in (1, -1):
                if h < PARTS - 1:
                    pass_z(z, h, sign)
                else:
                    @pl.when(jnp.logical_not(late(z, sign)))
                    def _():
                        pass_z(z, h, sign)
            spread(me, h)
            act(e_copy(me, h, sib), False)

    def own_late(sign):
        @pl.when(late(z, sign))
        def _():
            pass_z(z, PARTS - 1, sign)

    def take(zz, h, sign):
        blk = slot(zz, y, c)
        e_copy(blk, h, me).wait_recv()
        pass_z(zz, h, sign)
        act(e_copy(blk, h, sib), False)

    reach = jnp.maximum(jnp.where(k > 0, z, 0), jnp.where(k < states - 1, nz - 1 - z, 0))

    def natural(i, wanted, parts=range(PARTS)):
        for h in parts:
            for sign in (1, -1):
                zz = z - sign * i
                kept = owner_of(zz) == k
                mine_now = kept if wanted else jnp.logical_not(kept)
                if wanted and h == PARTS - 1:
                    mine_now = both(mine_now, jnp.logical_not(late(zz, sign)))

                @pl.when(both(within(zz), mine_now))
                def _():
                    take(zz, h, sign)
                    if wanted and i < nz - 2:
                        @pl.when(jnp.logical_or(late(zz, sign), reach <= i))
                        def _():
                            spread(slot(zz, y, c), h)
                    else:
                        spread(slot(zz, y, c), h)

    def deferred():
        for i in range(1, nz - 2):
            for sign in (1, -1):
                zz = z - sign * i

                @pl.when(both(within(zz), owner_of(zz) == k, reach > i, jnp.logical_not(late(zz, sign))))
                def _():
                    for h in range(PARTS):
                        spread(slot(zz, y, c), h)

    def delayed():
        for i in range(1, nz):
            for sign in (1, -1):
                zz = z - sign * i

                @pl.when(both(within(zz), late(zz, sign)))
                def _():
                    take(zz, PARTS - 1, sign)
                    spread(slot(zz, y, c), PARTS - 1)

    def rows_sent():
        for h in range(PARTS):
            for i in range(nz):
                for sign in (1, -1):
                    zz = z - sign * i

                    @pl.when(within(zz))
                    def _():
                        pass_z(zz, h, sign, drain=True)
                        if i or sign > 0:
                            spread(slot(zz, y, c), h, drain=True)
                            act(e_copy(slot(zz, y, c), h, sib), True)

    def across(j, drain=False):
        zz = turn(j)
        for h in range(PARTS):
            for u in range(1, ny):
                for sign in (1, -1):
                    yy = y - sign * u
                    onward = y + sign

                    @pl.when(both(yy >= 0, yy < ny))
                    def _():
                        blk = slot(zz, yy, c)
                        if not drain:
                            e_copy(blk, h, me).wait_recv()

                        @pl.when(both(onward >= 0, onward < ny))
                        def _():
                            act(e_copy(blk, h, slot(z, onward, c)), drain)

                        act(e_copy(blk, h, sib), drain)

    def sibling(j):
        zz = turn(j)
        for h in range(PARTS):
            for yy in range(ny):
                e_copy(slot(zz, yy, 1 - c), h, me).wait_recv()


    def unpack():
        for s in range(phys):
            plain = raw[:, s, :]
            for h in range(nch):
                for q in range(bpc):
                    at = column_of(h, q) * w
                    abuf[h, z, s, c, :, q * w : (q + 1) * w] = plain[:, at : at + w]

    def a_copy(h, zz, cc, dest):
        ref = abuf.at[h, zz, :, cc]
        return remote(ref, ref, a_send, a_recv.at[h, zz, cc], k, dest)

    def a_own(sign, drain=False):
        @pl.loop(0 if drain else jnp.where(late(z, sign), 1, 0), nch)
        def _(h):
            act(a_copy(h, z, c, slot(z + sign, y, c)), drain)

    def a_first():
        for sign in (1, -1):
            @pl.when(both(within(z + sign), late(z, sign)))
            def _():
                a_copy(0, z, c, slot(z + sign, y, c)).start()

    def a_edges(i, drain=False):
        @pl.when(both(z == i, z < nz - 1))
        def _():
            if not drain:
                own_late(1)
            a_own(1, drain)

        @pl.when(both(nz - 1 - z == i, z > 0))
        def _():
            if not drain:
                own_late(-1)
            a_own(-1, drain)

    def a_sibling(drain=False):
        @pl.loop(0, nch)
        def _(h):
            act(a_copy(h, z, c, sib), drain)

    def a_pass(h, i, drain=False):
        for sign in (1, -1):
            zz = z - sign * i
            onward = z + sign

            @pl.when(both(zz >= 0, zz < nz, onward >= 0, onward < nz))
            def _():
                if not drain:
                    a_copy(h, zz, c, me).wait_recv()
                act(a_copy(h, zz, c, slot(onward, y, c)), drain)
                act(a_copy(h, zz, c, sib), drain)

    def a_last(h, i, drain=False):
        for sign in (1, -1):
            zz = z - sign * i
            onward = z + sign

            @pl.when(both(zz >= 0, zz < nz, jnp.logical_or(onward < 0, onward >= nz)))
            def _():
                if not drain:
                    a_copy(h, zz, c, me).wait_recv()
                act(a_copy(h, zz, c, sib), drain)

    def a_ready(h):
        for zz in range(nz):
            a_copy(h, zz, 1 - c, me).wait_recv()


    def c_copy(zz, peer):
        ref = cbuf.at[pl.ds(zz * tpp, tpp)]
        return remote(ref, ref, c_send, c_recv, peer, me)

    def share(drain=False):
        for other in range(1, states):
            peer = lax.rem(k + other, states)
            zz = turn_of(peer, nz - 2)

            @pl.when(owner_of(zz) == k)
            def _():
                act(c_copy(zz, peer), drain)


    def p_copy(g, part_of, peer):
        return remote(
            psend.at[g, part_of], precv.at[k, lax.rem(g, gpp), part_of],
            p_send, p_recv.at[k, lax.div(g, tpp)], peer, me,
        )

    def span(zz):
        return pl.ds(pl.multiple_of(zz * piece, 128), piece)

    def my_copy(zz, yy):
        return remote(
            mown.at[zz, yy], mbuf.at[k, y, :, span(zz)], my_send, my_recv.at[zz, y], k, slot(z, yy, c)
        )

    def mx_copy(zz, yy, peer):
        ref = mbuf.at[k, yy, :, span(zz)]
        return remote(ref, ref, mx_send, mx_recv.at[k], peer, me)

    def flat_of(kk, at):
        return precv[kk, at].reshape(pairs * w, TILE).astype(jnp.float32)

    def halves(whole):
        return whole.astype(jnp.bfloat16).reshape(PARTS, pairs * w // PARTS, TILE)

    def tally(kk, g, whole):
        here = cbuf[g].reshape(pairs * w, TILE).astype(jnp.float32)
        line[kk] += jnp.sum((whole * here).reshape(pairs * w // 8, 8, TILE), axis=0)

    def p_wait(use):
        for i in range(nz // states):
            zz = k * (nz // states) + i
            for other in range(1, states):
                peer = lax.rem(k + other, states)
                counted = zz == turn_of(peer, nz - 2)

                @pl.when(jnp.logical_not(counted) if use else counted)
                def _():
                    ref = precv.at[peer, pl.ds(i * tpp, tpp)]
                    remote(ref, ref, p_send, p_recv.at[peer, zz], peer, me).wait_recv()
                    if use:
                        @pl.loop(0, tpp)
                        def _(r):
                            tally(peer, zz * tpp + r, flat_of(peer, i * tpp + r))

    def project(j):
        zz = turn(j)

        if j == nz - 2:
            @pl.when(owner_of(zz) != k)
            def _():
                c_copy(zz, k).wait_recv()

        @pl.loop(0, tpp)
        def _(r):
            g = zz * tpp + r
            left = ebuf[pl.ds(g * per_group, per_group)].reshape(TILE, width)
            prod = lax.dot_general(
                stored[...], left, (((1,), (1,)), ((), ())), preferred_element_type=jnp.float32
            )
            for q in range(cpt):
                yy = r * cpt + q
                moved = jnp.concatenate(
                    [
                        prod[(pairs + s) * w : (pairs + s + 1) * w, q * cell : (q + 1) * cell]
                        for s in range(phys)
                    ],
                    axis=1,
                ).astype(jnp.bfloat16)

                @pl.when(yy == y)
                def _():
                    mbuf[k, y, :, span(zz)] = moved
                    for other in range(1, states):
                        mx_copy(zz, y, lax.rem(k + other, states)).start()

                @pl.when(yy != y)
                def _():
                    mown[zz, yy] = moved
                    if j >= nz - 2:
                        my_copy(zz, yy).start()

            whole = prod[: pairs * w]
            owner = lax.div(g, gpp)

            @pl.when(jnp.logical_or(owner == k, j == nz - 2))
            def _():
                tally(k, g, whole)

            @pl.when(owner == k)
            def _():
                precv[k, lax.rem(g, gpp)] = halves(whole)

            @pl.when(owner != k)
            def _():
                psend[g] = halves(whole)

    def hand_over(j, n, drain=False):
        zz = turn(j)
        g = zz * tpp + n // PARTS
        for other in range(1, states):
            peer = lax.rem(k + other, states)

            @pl.when(lax.div(g, gpp) == peer)
            def _():
                act(p_copy(g, n % PARTS, peer), drain)

    def forward(j, drain=False):
        zz = turn(j)
        for u in range(1, ny):
            yy = lax.rem(y + u, ny)
            if not drain:
                ref = mbuf.at[k, yy, :, span(zz)]
                remote(ref, ref, my_send, my_recv.at[zz, yy], k, me).wait_recv()
            for other in range(1, states):
                act(mx_copy(zz, yy, lax.rem(k + other, states)), drain)


    def t_copy(zc, yy):
        return remote(
            part.at[zc, yy], prt.at[zc, y], t_send, t_recv.at[zc, y], k, slot(z, yy, c)
        )

    def grow(h):
        total = jnp.dot(
            mbuf[...].reshape(ecols, nz * piece),
            abuf[h].reshape(nz * piece, fch),
            preferred_element_type=jnp.float32,
        )
        for q in range(bpc):
            if direct:
                zc, yy = h, q
            else:
                fb = h * bpc + q
                zc = lax.div(fb, ny * nc) * nc + lax.rem(fb, nc)
                yy = lax.rem(lax.div(fb, nc), ny)
            block = total[:, q * w : (q + 1) * w]

            @pl.when(yy == y)
            def _():
                acc[zc] = block

            @pl.when(yy != y)
            def _():
                part[zc, yy] = block.astype(jnp.bfloat16)
                t_copy(zc, yy).start()

    def target(kk, zc):
        return slot(kk * (nz // states) + lax.div(zc, nc), y, lax.rem(zc, nc))

    def place(src):
        if direct:
            return next_ref.at[:, pl.ds(pl.multiple_of(src * w, 128), w)]
        return next_ref.at[src]


    def n_copy(kk, zc, yy):
        return remote(
            nbuf.at[kk, zc, yy], place(slot(z, yy, c)), n_send, n_recv, k, target(kk, zc)
        )

    def deliver(kk, zc, drain=False):
        stays = target(kk, zc) == me
        for yy in range(ny):
            if not drain:
                @pl.when(stays)
                def _():
                    place(slot(z, yy, c))[...] = nbuf[kk, zc, yy]

            @pl.when(jnp.logical_not(stays))
            def _():
                act(n_copy(kk, zc, yy), drain)

    def r_copy(kk, zc):
        return remote(nsend.at[kk, zc], nbuf.at[k, zc], r_send, r_recv.at[k, zc], kk, me)

    def finish(zc):
        total = acc[zc]
        for u in range(1, ny):
            yy = lax.rem(y + u, ny)
            ref = prt.at[zc, yy]
            remote(ref, ref, t_send, t_recv.at[zc, yy], k, me).wait_recv()
            total = total + ref[...].astype(jnp.float32)
        for kk in range(states):
            blocks = [
                total[(kk * ny + yy) * w : (kk * ny + yy + 1) * w].T.astype(jnp.bfloat16)
                for yy in range(ny)
            ]

            @pl.when(kk == k)
            def _():
                for yy in range(ny):
                    nbuf[k, zc, yy] = blocks[yy]
                deliver(k, zc)

            @pl.when(kk != k)
            def _():
                for yy in range(ny):
                    nsend[kk, zc, yy] = blocks[yy]
                r_copy(kk, zc).start()

    def pass_on(zc):
        for other in range(1, states):
            kk = lax.rem(k + other, states)
            ref = nbuf.at[kk, zc]
            remote(ref, ref, r_send, r_recv.at[kk, zc], k, me).wait_recv()
            deliver(kk, zc)


    def i_near(u):
        there = lax.rem(lax.rem(me, near) + u, near)
        ref = iplane.at[lax.rem(me, near)]
        return remote(ref, ref, i_send.at[0], i_recv.at[0], k, z * near + there)

    def i_far(u):
        ref = iline.at[z]
        return remote(ref, ref, i_send.at[1], i_recv.at[1], k, slot(lax.rem(z + u, nz), y, c))

    def i_peer(u):
        ref = istate.at[k]
        return remote(ref, ref, i_send.at[2], i_recv.at[2], lax.rem(k + u, states), me)

    stages = ((i_near, near, iplane), (i_far, nz, iline), (i_peer, states, istate))

    def start(n):
        send, number, _ = stages[n]
        for u in range(1, number):
            send(u).start()

    def gathered(n):
        _, number, buf = stages[n]
        rest = buf.at[pl.ds(0, number - 1)]
        remote(rest, rest, i_send.at[n], i_recv.at[n], k, me).wait_recv()

    def overlap(n):
        if n == 0:
            for kk in range(states):
                short = jnp.sum(line[kk], axis=0, keepdims=True)
                total = short[:, :128]
                for at in range(128, TILE, 128):
                    total = total + short[:, at : at + 128]
                iplane[lax.rem(me, near), kk : kk + 1] = total
        elif n == 1:
            gathered(0)
            iline[z] = jnp.sum(iplane[...], axis=0)
        else:
            gathered(1)
            istate[k] = jnp.sum(iline[...], axis=0)
        start(n)

    def penalize():
        gathered(2)
        p_wait(False)
        scale = 1.0 / (phys * width)
        factors = [weight_ref[kk] * (jnp.sum(istate[:, kk]) * scale) for kk in range(states)]
        for g in range(gpp):
            value = cbuf[k * gpp + g].reshape(pairs * w, TILE).astype(jnp.float32)
            for kk in range(states):
                value = value + factors[kk] * flat_of(kk, g)
            pen_ref[:, :, g * TILE : (g + 1) * TILE] = value.reshape(pairs, w, TILE)

    line[...] = jnp.zeros_like(line)
    e_load.wait()
    for i in range(nz + 1):
        if i == 0:
            own()
            a_load.wait()
            unpack()
            a_first()
            a_sibling()
        elif i < nz:
            if i < nz - 1:
                natural(i, False)
            if i == nz - 2:
                natural(nz - 1, False, range(PARTS - 1))
                deferred()
            if i == nz - 1:
                natural(nz - 1, False, [PARTS - 1])
            natural(i, True)
            if i == nz - 1:
                delayed()
        if i < nz:
            a_edges(i)
            if i == 0:
                for copy in c_loads:
                    copy.wait()
                share()
        if i == nz - 1:
            for j in range(nz - 2):
                for u in range(1, ny):
                    my_copy(turn(j), lax.rem(y + u, ny)).start()

            @pl.loop(0, nch)
            def _(h):
                a_pass(h, 1)
        if i >= 1:
            across(i - 1)
            sibling(i - 1)
            if i == 1:
                for copy in loads:
                    copy.wait()
            project(i - 1)
            if i - 1 < nz - 2:
                for n in range(slices):
                    hand_over(i - 1, n)

    for i in range(2, nz):
        @pl.loop(0, nch)
        def _(h):
            a_pass(h, i)

    for j in range(nz):
        forward(j)
    p_wait(True)
    overlap(0)
    rows_sent()
    for i in range(nz):
        across(i, drain=True)
    for i in range(1, nz - 1):
        @pl.loop(0, nch)
        def _(h):
            a_last(h, i)
    a_last(0, nz - 1)
    for other in range(1, states):
        peer = lax.rem(k + other, states)
        ref = mbuf.at[peer]
        remote(ref, ref, mx_send, mx_recv.at[peer], peer, me).wait_recv()

    @pl.loop(0, nch)
    def _(h):
        a_ready(h)
        grow(h)

        @pl.when(h == 0)
        def _():
            overlap(1)

        for n in range(slices - 1):
            @pl.when(h == (min(n, nch - 1) if n < slices - 2 else nch - 1))
            def _():
                hand_over(nz - 2, n)
                hand_over(nz - 1, n)

        @pl.when(h < nch - 1)
        def _():
            a_last(h + 1, nz - 1)

        @pl.when(h == nch - 1)
        def _():
            overlap(2)

        if direct:
            @pl.when(h > 1)
            def _():
                finish(h - 2)

    if direct:
        pass_on(0)
        finish(nch - 2)
        hand_over(nz - 2, slices - 1)
        hand_over(nz - 1, slices - 1)
        for h in range(1, nch - 2):
            pass_on(h)
        finish(nch - 1)
        for h in range(max(nch - 2, 1), nch):
            pass_on(h)
    else:
        hand_over(nz - 2, slices - 1)
        hand_over(nz - 1, slices - 1)


        @pl.loop(0, mine)
        def _(zc):
            finish(zc)

        @pl.loop(0, mine)
        def _(zc):
            pass_on(zc)

    penalize()
    for i in range(nz):
        a_edges(i, drain=True)
    a_sibling(drain=True)

    @pl.loop(0, nch)
    def _(h):
        for i in range(1, nz):
            a_pass(h, i, drain=True)
            a_last(h, i, drain=True)

    for i in range(nz):
        forward(i, drain=True)
        for n in range(slices):
            hand_over(i, n, drain=True)

    @pl.loop(0, nz)
    def _(zz):
        for u in range(1, ny):
            my_copy(zz, lax.rem(y + u, ny)).wait_send()
        for other in range(1, states):
            mx_copy(zz, y, lax.rem(k + other, states)).wait_send()

    share(drain=True)
    for send, number, _ in stages:
        for u in range(1, number):
            send(u).wait_send()

    @pl.loop(0, mine)
    def _(zc):
        for u in range(1, ny):
            t_copy(zc, lax.rem(y + u, ny)).wait_send()
        for kk in range(states):
            @pl.when(kk != k)
            def _():
                r_copy(kk, zc).wait_send()

            deliver(kk, zc, drain=True)

    if direct:
        rest = next_ref.at[:, pl.ds(0, (bonds - ny) * w)]
    else:
        rest = next_ref.at[pl.ds(0, bonds - ny)]
    remote(rest, rest, n_send, n_recv, k, me).wait_recv()


def shards(states, bonds, intersect_left, stored_block, stored_site, current_site, current_block, penalty_weight):
    rows, width = intersect_left.shape[1:]
    pairs, w = stored_block.shape[1:3]
    phys = stored_site.shape[1]
    fwidth = current_site.shape[2]
    groups = width // TILE
    gpp = groups // states
    ny = 1
    while 4 * ny * ny <= bonds // CORES:
        ny *= 2
    nz = bonds // (CORES * ny)
    direct = w % 128 == 0
    fch = ny * w if direct else max(w, 128)
    nch, mine = fwidth // fch, fwidth // w // ny
    cell = CORES * rows
    piece = phys * cell
    bf, f32 = jnp.bfloat16, jnp.float32
    anywhere = pl.BlockSpec(memory_space=pltpu.HBM)
    dma = pltpu.SemaphoreType.DMA
    penalized, grown = pl.pallas_call(
        functools.partial(kernel, states, bonds, ny, fch),
        out_shape=(
            pltpu.VMEM(current_block.shape, f32),
            pltpu.VMEM((w, bonds * w) if direct else (bonds, w, w), bf),
        ),
        in_specs=[anywhere] * 5 + [pl.BlockSpec(memory_space=pltpu.SMEM)],
        out_specs=(pl.BlockSpec(memory_space=pltpu.VMEM),) * 2,
        scratch_shapes=[
            pltpu.VMEM((bonds, PARTS, rows // PARTS, width), bf),
            pltpu.VMEM((rows, phys, fwidth), bf),
            pltpu.VMEM((nch, nz, phys, CORES, rows, fch), bf),
            pltpu.VMEM(((pairs + phys) * w, width), bf),
            pltpu.VMEM((groups, pairs, w, TILE), bf),
            pltpu.VMEM((groups, PARTS, pairs * w // PARTS, TILE), bf),
            pltpu.VMEM((states, gpp, PARTS, pairs * w // PARTS, TILE), bf),
            pltpu.VMEM((nz, ny, w, piece), bf),
            pltpu.VMEM((states, ny, w, nz * piece), bf),
            pltpu.VMEM((mine, states * ny * w, w), f32),
            pltpu.VMEM((mine, ny, states * ny * w, w), bf),
            pltpu.VMEM((mine, ny, states * ny * w, w), bf),
            pltpu.VMEM((states, mine, ny, w, w), bf),
            pltpu.VMEM((states, mine, ny, w, w), bf),
            pltpu.VMEM((CORES * ny, states, 128), f32),
            pltpu.VMEM((nz, states, 128), f32),
            pltpu.VMEM((states, states, 128), f32),
            pltpu.VMEM((states, 8, TILE), f32),
            dma((4,)),
            dma, dma((bonds, PARTS)),
            dma, dma((nch, nz, CORES)),
            dma, dma((states, nz)),
            dma, dma((nz, ny)),
            dma, dma((states,)),
            dma, dma,
            dma((3,)), dma((3,)),
            dma, dma((mine, ny)),
            dma, dma((states, mine)),
            dma, dma,
        ],
        compiler_params=pltpu.CompilerParams(
            collective_id=0, has_side_effects=True, vmem_limit_bytes=60 * 1024 * 1024
        ),
    )(
        intersect_left.reshape(PARTS, rows // PARTS, width), stored_block[0], stored_site[0],
        current_site, current_block, penalty_weight,
    )
    if direct:
        return penalized, grown[None]
    return penalized, grown.transpose(1, 0, 2).reshape(1, w, bonds * w)


def solution(mesh):
    placed = (
        P("state", "bond", None),
        P("state", None, "bond", None),
        P("state", None, "bond", None),
        P("bond", None, "state"),
        P(None, "bond", "state"),
        P(),
    )
    return jax.shard_map(
        functools.partial(shards, mesh.shape["state"], mesh.shape["bond"]),
        mesh=mesh,
        in_specs=placed,
        out_specs=(P(None, "bond", "state"), P("state", "bond", None)),
        check_vma=False,
    )
```

```python
import functools

import jax
import jax.numpy as jnp
from jax import lax
from jax.experimental import pallas as pl
from jax.experimental.pallas import tpu as pltpu
from jax.sharding import PartitionSpec as P

MESH = pl.DeviceIdType.MESH
CORES = 2
TILE = 256
PARTS = 2


def both(*conds):
    return functools.reduce(jnp.logical_and, conds)


def kernel(
    states, bonds, rows_y, fch,
    env_hbm, block_hbm, site_hbm, grow_hbm, current_hbm, weight_ref,
    pen_ref, next_ref,
    ebuf, raw, abuf, stored, cbuf, psend, precv, mown, mbuf, acc, part, prt, nsend, nbuf, iplane, iline, istate, line,
    local_sem, e_send, e_recv, a_send, a_recv, p_send, p_recv, my_send, my_recv, mx_send, mx_recv,
    c_send, c_recv, i_send, i_recv, t_send, t_recv, r_send, r_recv, n_send, n_recv,
):
    nc, ny = CORES, rows_y
    nz = bonds // (nc * ny)
    hr, width = ebuf.shape[2:]
    rows = hr * PARTS
    pairs, w = block_hbm.shape[:2]
    phys = site_hbm.shape[0]
    fwidth = grow_hbm.shape[2]
    nch = fwidth // fch
    bpc = fch // w
    fbs = fwidth // w
    mine = fbs // ny
    cell = nc * rows
    per_group = TILE // rows
    tpp = ny * cell // TILE
    cpt = TILE // cell
    groups = width // TILE
    gpp = groups // states
    ecols = states * ny * w
    direct = w % 128 == 0
    piece = phys * cell

    k = lax.axis_index("state")
    me = lax.axis_index("bond")
    c = lax.rem(me, nc)
    y = lax.rem(lax.div(me, nc), ny)
    z = lax.div(me, nc * ny)
    near = ny * nc
    slices = PARTS * tpp

    def slot(zz, yy, cc):
        return (zz * ny + yy) * nc + cc

    sib = slot(z, y, 1 - c)

    def owner_of(zz):
        return lax.div(zz * tpp, gpp)

    def order(kk, zz):
        rest = sorted(set(range(nz)) - {zz}, key=lambda other: abs(other - zz))
        return [zz] + sorted(rest, key=lambda other: other * tpp // gpp == kk)

    def turn_of(kk, j):
        at = jnp.int32(0)
        for k_ in range(states):
            for z_ in range(nz):
                at = at + jnp.where(both(kk == k_, z == z_), order(k_, z_)[j], 0)
        return at

    turns = [turn_of(k, j) for j in range(nz)]

    def turn(j):
        return turns[j]

    def column_of(h, q):
        if direct:
            return (h // nc * ny + q) * nc + h % nc
        return h * bpc + q

    e_load = pltpu.make_async_copy(env_hbm, ebuf.at[me], local_sem.at[0])
    e_load.start()
    a_load = pltpu.make_async_copy(grow_hbm, raw, local_sem.at[1])
    a_load.start()
    loads = []
    for q in range(pairs):
        loads.append(pltpu.make_async_copy(block_hbm.at[q], stored.at[pl.ds(q * w, w)], local_sem.at[2]))
    for s in range(phys):
        loads.append(
            pltpu.make_async_copy(site_hbm.at[s], stored.at[pl.ds((pairs + s) * w, w)], local_sem.at[2])
        )
    for copy in loads:
        copy.start()
    c_loads = [
        pltpu.make_async_copy(
            current_hbm.at[:, :, pl.ds(g * TILE, TILE)], cbuf.at[k * gpp + g], local_sem.at[3]
        )
        for g in range(gpp)
    ]
    for copy in c_loads:
        copy.start()

    barrier = pltpu.get_barrier_semaphore()

    def greet(kk, dest):
        pl.semaphore_signal(barrier, inc=1, device_id=(kk, dest), device_id_type=MESH)

    @pl.when(z > 0)
    def _():
        greet(k, slot(z - 1, y, c))

    @pl.when(z < nz - 1)
    def _():
        greet(k, slot(z + 1, y, c))

    for other in range(1, near):
        greet(k, z * near + lax.rem(lax.rem(me, near) + other, near))
    for other in range(1, states):
        greet(lax.rem(k + other, states), me)
    ends = jnp.where(z > 0, 1, 0) + jnp.where(z < nz - 1, 1, 0)
    pl.semaphore_wait(barrier, near + states - 2 + ends)

    def remote(src, dst, ss, rs, kk, dest):
        return pltpu.make_async_remote_copy(
            src_ref=src, dst_ref=dst, send_sem=ss, recv_sem=rs, device_id=(kk, dest), device_id_type=MESH
        )

    def act(copy, drain):
        if drain:
            copy.wait_send()
        else:
            copy.start()


    def e_copy(blk, h, dest):
        ref = ebuf.at[blk, h]
        return remote(ref, ref, e_send, e_recv.at[blk, h], k, dest)

    def spread(blk, h, drain=False):
        @pl.when(y > 0)
        def _():
            act(e_copy(blk, h, slot(z, y - 1, c)), drain)

        @pl.when(y < ny - 1)
        def _():
            act(e_copy(blk, h, slot(z, y + 1, c)), drain)

    def within(zz):
        return both(zz >= 0, zz < nz)


    def late(zz, sign):
        return both(owner_of(zz) == k, k != (0 if sign > 0 else states - 1))

    def pass_z(zz, h, sign, drain=False):
        @pl.when(within(z + sign))
        def _():
            act(e_copy(slot(zz, y, c), h, slot(z + sign, y, c)), drain)

    def own():
        for h in range(PARTS):
            for sign in (1, -1):
                if h < PARTS - 1:
                    pass_z(z, h, sign)
                else:
                    @pl.when(jnp.logical_not(late(z, sign)))
                    def _():
                        pass_z(z, h, sign)
            spread(me, h)
            act(e_copy(me, h, sib), False)

    def own_late(sign):
        @pl.when(late(z, sign))
        def _():
            pass_z(z, PARTS - 1, sign)

    def take(zz, h, sign):
        blk = slot(zz, y, c)
        e_copy(blk, h, me).wait_recv()
        pass_z(zz, h, sign)
        act(e_copy(blk, h, sib), False)

    reach = jnp.maximum(jnp.where(k > 0, z, 0), jnp.where(k < states - 1, nz - 1 - z, 0))

    def natural(i, wanted, parts=range(PARTS)):
        for h in parts:
            for sign in (1, -1):
                zz = z - sign * i
                kept = owner_of(zz) == k
                mine_now = kept if wanted else jnp.logical_not(kept)
                if wanted and h == PARTS - 1:
                    mine_now = both(mine_now, jnp.logical_not(late(zz, sign)))

                @pl.when(both(within(zz), mine_now))
                def _():
                    take(zz, h, sign)
                    if wanted and i < nz - 2:
                        @pl.when(jnp.logical_or(late(zz, sign), reach <= i))
                        def _():
                            spread(slot(zz, y, c), h)
                    else:
                        spread(slot(zz, y, c), h)

    def deferred():
        for i in range(1, nz - 2):
            for sign in (1, -1):
                zz = z - sign * i

                @pl.when(both(within(zz), owner_of(zz) == k, reach > i, jnp.logical_not(late(zz, sign))))
                def _():
                    for h in range(PARTS):
                        spread(slot(zz, y, c), h)

    def delayed():
        for i in range(1, nz):
            for sign in (1, -1):
                zz = z - sign * i

                @pl.when(both(within(zz), late(zz, sign)))
                def _():
                    take(zz, PARTS - 1, sign)
                    spread(slot(zz, y, c), PARTS - 1)

    def rows_sent():
        for h in range(PARTS):
            for i in range(nz):
                for sign in (1, -1):
                    zz = z - sign * i

                    @pl.when(within(zz))
                    def _():
                        pass_z(zz, h, sign, drain=True)
                        if i or sign > 0:
                            spread(slot(zz, y, c), h, drain=True)
                            act(e_copy(slot(zz, y, c), h, sib), True)

    def across(j, drain=False):
        zz = turn(j)
        for h in range(PARTS):
            for u in range(1, ny):
                for sign in (1, -1):
                    yy = y - sign * u
                    onward = y + sign

                    @pl.when(both(yy >= 0, yy < ny))
                    def _():
                        blk = slot(zz, yy, c)
                        if not drain:
                            e_copy(blk, h, me).wait_recv()

                        @pl.when(both(onward >= 0, onward < ny))
                        def _():
                            act(e_copy(blk, h, slot(z, onward, c)), drain)

                        act(e_copy(blk, h, sib), drain)

    def sibling(j):
        zz = turn(j)
        for h in range(PARTS):
            for yy in range(ny):
                e_copy(slot(zz, yy, 1 - c), h, me).wait_recv()


    def unpack():
        for s in range(phys):
            plain = raw[:, s, :]
            for h in range(nch):
                for q in range(bpc):
                    at = column_of(h, q) * w
                    abuf[h, z, s, c, :, q * w : (q + 1) * w] = plain[:, at : at + w]

    def a_copy(h, zz, cc, dest):
        ref = abuf.at[h, zz, :, cc]
        return remote(ref, ref, a_send, a_recv.at[h, zz, cc], k, dest)

    def a_own(sign, drain=False):
        @pl.loop(0 if drain else jnp.where(late(z, sign), 1, 0), nch)
        def _(h):
            act(a_copy(h, z, c, slot(z + sign, y, c)), drain)

    def a_first():
        for sign in (1, -1):
            @pl.when(both(within(z + sign), late(z, sign)))
            def _():
                a_copy(0, z, c, slot(z + sign, y, c)).start()

    def a_edges(i, drain=False):
        @pl.when(both(z == i, z < nz - 1))
        def _():
            if not drain:
                own_late(1)
            a_own(1, drain)

        @pl.when(both(nz - 1 - z == i, z > 0))
        def _():
            if not drain:
                own_late(-1)
            a_own(-1, drain)

    def a_sibling(drain=False):
        @pl.loop(0, nch)
        def _(h):
            act(a_copy(h, z, c, sib), drain)

    def a_pass(h, i, drain=False):
        for sign in (1, -1):
            zz = z - sign * i
            onward = z + sign

            @pl.when(both(zz >= 0, zz < nz, onward >= 0, onward < nz))
            def _():
                if not drain:
                    a_copy(h, zz, c, me).wait_recv()
                act(a_copy(h, zz, c, slot(onward, y, c)), drain)
                act(a_copy(h, zz, c, sib), drain)

    def a_last(h, i, drain=False):
        for sign in (1, -1):
            zz = z - sign * i
            onward = z + sign

            @pl.when(both(zz >= 0, zz < nz, jnp.logical_or(onward < 0, onward >= nz)))
            def _():
                if not drain:
                    a_copy(h, zz, c, me).wait_recv()
                act(a_copy(h, zz, c, sib), drain)

    def a_ready(h):
        for zz in range(nz):
            a_copy(h, zz, 1 - c, me).wait_recv()


    def c_copy(zz, peer):
        ref = cbuf.at[pl.ds(zz * tpp, tpp)]
        return remote(ref, ref, c_send, c_recv, peer, me)

    def share(drain=False):
        for other in range(1, states):
            peer = lax.rem(k + other, states)
            zz = turn_of(peer, nz - 2)

            @pl.when(owner_of(zz) == k)
            def _():
                act(c_copy(zz, peer), drain)


    def p_copy(g, part_of, peer):
        return remote(
            psend.at[g, part_of], precv.at[k, lax.rem(g, gpp), part_of],
            p_send, p_recv.at[k, lax.div(g, tpp)], peer, me,
        )

    def span(zz):
        return pl.ds(pl.multiple_of(zz * piece, 128), piece)

    def my_copy(zz, yy):
        return remote(
            mown.at[zz, yy], mbuf.at[k, y, :, span(zz)], my_send, my_recv.at[zz, y], k, slot(z, yy, c)
        )

    def mx_copy(zz, yy, peer):
        ref = mbuf.at[k, yy, :, span(zz)]
        return remote(ref, ref, mx_send, mx_recv.at[k], peer, me)

    def flat_of(kk, at):
        return precv[kk, at].reshape(pairs * w, TILE).astype(jnp.float32)

    def halves(whole):
        return whole.astype(jnp.bfloat16).reshape(PARTS, pairs * w // PARTS, TILE)

    def tally(kk, g, whole):
        here = cbuf[g].reshape(pairs * w, TILE).astype(jnp.float32)
        line[kk] += jnp.sum((whole * here).reshape(pairs * w // 8, 8, TILE), axis=0)

    def p_wait(use):
        for i in range(nz // states):
            zz = k * (nz // states) + i
            for other in range(1, states):
                peer = lax.rem(k + other, states)
                counted = zz == turn_of(peer, nz - 2)

                @pl.when(jnp.logical_not(counted) if use else counted)
                def _():
                    ref = precv.at[peer, pl.ds(i * tpp, tpp)]
                    remote(ref, ref, p_send, p_recv.at[peer, zz], peer, me).wait_recv()
                    if use:
                        @pl.loop(0, tpp)
                        def _(r):
                            tally(peer, zz * tpp + r, flat_of(peer, i * tpp + r))

    def project(j):
        zz = turn(j)

        if j == nz - 2:
            @pl.when(owner_of(zz) != k)
            def _():
                c_copy(zz, k).wait_recv()

        @pl.loop(0, tpp)
        def _(r):
            g = zz * tpp + r
            left = ebuf[pl.ds(g * per_group, per_group)].reshape(TILE, width)
            prod = lax.dot_general(
                stored[...], left, (((1,), (1,)), ((), ())), preferred_element_type=jnp.float32
            )
            for q in range(cpt):
                yy = r * cpt + q
                moved = jnp.concatenate(
                    [
                        prod[(pairs + s) * w : (pairs + s + 1) * w, q * cell : (q + 1) * cell]
                        for s in range(phys)
                    ],
                    axis=1,
                ).astype(jnp.bfloat16)

                @pl.when(yy == y)
                def _():
                    mbuf[k, y, :, span(zz)] = moved
                    for other in range(1, states):
                        mx_copy(zz, y, lax.rem(k + other, states)).start()

                @pl.when(yy != y)
                def _():
                    mown[zz, yy] = moved
                    if j >= nz - 2:
                        my_copy(zz, yy).start()

            whole = prod[: pairs * w]
            owner = lax.div(g, gpp)

            @pl.when(jnp.logical_or(owner == k, j == nz - 2))
            def _():
                tally(k, g, whole)

            @pl.when(owner == k)
            def _():
                precv[k, lax.rem(g, gpp)] = halves(whole)

            @pl.when(owner != k)
            def _():
                psend[g] = halves(whole)

    def hand_over(j, n, drain=False):
        zz = turn(j)
        g = zz * tpp + n // PARTS
        for other in range(1, states):
            peer = lax.rem(k + other, states)

            @pl.when(lax.div(g, gpp) == peer)
            def _():
                act(p_copy(g, n % PARTS, peer), drain)

    def forward(j, drain=False):
        zz = turn(j)
        for u in range(1, ny):
            yy = lax.rem(y + u, ny)
            if not drain:
                ref = mbuf.at[k, yy, :, span(zz)]
                remote(ref, ref, my_send, my_recv.at[zz, yy], k, me).wait_recv()
            for other in range(1, states):
                act(mx_copy(zz, yy, lax.rem(k + other, states)), drain)


    def t_copy(zc, yy, kk):
        return remote(
            part.at[zc, yy, kk], prt.at[zc, y, kk], t_send, t_recv.at[zc, y, kk], k, slot(z, yy, c)
        )

    def parts_of(h):
        for q in range(bpc):
            if direct:
                yield q, h, q
            else:
                fb = h * bpc + q
                yield (
                    q,
                    lax.div(fb, ny * nc) * nc + lax.rem(fb, nc),
                    lax.rem(lax.div(fb, nc), ny),
                )

    def store(zc, yy, kk, block):
        @pl.when(yy == y)
        def _():
            acc[zc, kk] = block

        @pl.when(yy != y)
        def _():
            part[zc, yy, kk] = block.astype(jnp.bfloat16)

    def grow(h, kk):
        total = jnp.dot(
            mbuf[kk].reshape(ny * w, nz * piece),
            abuf[h].reshape(nz * piece, fch),
            preferred_element_type=jnp.float32,
        )
        for q, zc, yy in parts_of(h):
            store(zc, yy, kk, total[:, q * w : (q + 1) * w])

            @pl.when(yy != y)
            def _():
                t_copy(zc, yy, kk).start()

    def grow_all(h):
        total = jnp.dot(
            mbuf[...].reshape(ecols, nz * piece),
            abuf[h].reshape(nz * piece, fch),
            preferred_element_type=jnp.float32,
        )
        for q, zc, yy in parts_of(h):
            for kk in range(states):
                store(zc, yy, kk, total[kk * ny * w : (kk + 1) * ny * w, q * w : (q + 1) * w])

            @pl.when(yy != y)
            def _():
                for other in range(1, states + 1):
                    t_copy(zc, yy, lax.rem(k + other, states)).start()

    def grow_others(h):
        @pl.loop(1, states)
        def _(other):
            grow(h, lax.rem(k + other, states))

    def target(kk, zc):
        return slot(kk * (nz // states) + lax.div(zc, nc), y, lax.rem(zc, nc))

    def place(src):
        if direct:
            return next_ref.at[:, pl.ds(pl.multiple_of(src * w, 128), w)]
        return next_ref.at[src]


    def n_copy(kk, zc, yy):
        return remote(
            nbuf.at[kk, zc, yy], place(slot(z, yy, c)), n_send, n_recv, k, target(kk, zc)
        )

    def deliver(kk, zc, drain=False):
        stays = target(kk, zc) == me
        for yy in range(ny):
            if not drain:
                @pl.when(stays)
                def _():
                    place(slot(z, yy, c))[...] = nbuf[kk, zc, yy]

            @pl.when(jnp.logical_not(stays))
            def _():
                act(n_copy(kk, zc, yy), drain)

    def r_copy(kk, zc):
        return remote(nsend.at[kk, zc], nbuf.at[k, zc], r_send, r_recv.at[k, zc], kk, me)

    def summed(zc, kk):
        total = acc[zc, kk]
        for u in range(1, ny):
            yy = lax.rem(y + u, ny)
            ref = prt.at[zc, yy, kk]
            remote(ref, ref, t_send, t_recv.at[zc, yy, kk], k, me).wait_recv()
            total = total + ref[...].astype(jnp.float32)
        return [total[yy * w : (yy + 1) * w].T.astype(jnp.bfloat16) for yy in range(ny)]

    def finish(zc):
        for other in range(1, states):
            kk = lax.rem(k + other, states)
            blocks = summed(zc, kk)
            for yy in range(ny):
                nsend[kk, zc, yy] = blocks[yy]
            r_copy(kk, zc).start()
        blocks = summed(zc, k)
        for yy in range(ny):
            nbuf[k, zc, yy] = blocks[yy]
        deliver(k, zc)

    def pass_on(zc):
        for other in range(1, states):
            kk = lax.rem(k + other, states)
            ref = nbuf.at[kk, zc]
            remote(ref, ref, r_send, r_recv.at[kk, zc], k, me).wait_recv()
            deliver(kk, zc)


    def i_near(u):
        there = lax.rem(lax.rem(me, near) + u, near)
        ref = iplane.at[lax.rem(me, near)]
        return remote(ref, ref, i_send.at[0], i_recv.at[0], k, z * near + there)

    def i_far(u):
        ref = iline.at[z]
        return remote(ref, ref, i_send.at[1], i_recv.at[1], k, slot(lax.rem(z + u, nz), y, c))

    def i_peer(u):
        ref = istate.at[k]
        return remote(ref, ref, i_send.at[2], i_recv.at[2], lax.rem(k + u, states), me)

    stages = ((i_near, near, iplane), (i_far, nz, iline), (i_peer, states, istate))

    def start(n):
        send, number, _ = stages[n]
        for u in range(1, number):
            send(u).start()

    def gathered(n):
        _, number, buf = stages[n]
        rest = buf.at[pl.ds(0, number - 1)]
        remote(rest, rest, i_send.at[n], i_recv.at[n], k, me).wait_recv()

    def overlap(n):
        if n == 0:
            for kk in range(states):
                short = jnp.sum(line[kk], axis=0, keepdims=True)
                total = short[:, :128]
                for at in range(128, TILE, 128):
                    total = total + short[:, at : at + 128]
                iplane[lax.rem(me, near), kk : kk + 1] = total
        elif n == 1:
            gathered(0)
            iline[z] = jnp.sum(iplane[...], axis=0)
        else:
            gathered(1)
            istate[k] = jnp.sum(iline[...], axis=0)
        start(n)

    def penalize():
        gathered(2)
        p_wait(False)
        scale = 1.0 / (phys * width)
        factors = [weight_ref[kk] * (jnp.sum(istate[:, kk]) * scale) for kk in range(states)]
        for g in range(gpp):
            value = cbuf[k * gpp + g].reshape(pairs * w, TILE).astype(jnp.float32)
            for kk in range(states):
                value = value + factors[kk] * flat_of(kk, g)
            pen_ref[:, :, g * TILE : (g + 1) * TILE] = value.reshape(pairs, w, TILE)

    line[...] = jnp.zeros_like(line)
    e_load.wait()
    for i in range(nz + 1):
        if i == 0:
            own()
            a_load.wait()
            unpack()
            a_first()
            a_sibling()
        elif i < nz:
            if i < nz - 1:
                natural(i, False)
            if i == nz - 2:
                natural(nz - 1, False, range(PARTS - 1))
                deferred()
            if i == nz - 1:
                natural(nz - 1, False, [PARTS - 1])
            natural(i, True)
            if i == nz - 1:
                delayed()
        if i < nz:
            a_edges(i)
            if i == 0:
                for copy in c_loads:
                    copy.wait()
                share()
        if i == nz - 1:
            for j in range(nz - 2):
                for u in range(1, ny):
                    my_copy(turn(j), lax.rem(y + u, ny)).start()

            @pl.loop(0, nch)
            def _(h):
                a_pass(h, 1)
        if i >= 1:
            across(i - 1)
            sibling(i - 1)
            if i == 1:
                for copy in loads:
                    copy.wait()
            project(i - 1)
            if i - 1 < nz - 2:
                for n in range(slices):
                    hand_over(i - 1, n)

    for i in range(2, nz):
        @pl.loop(0, nch)
        def _(h):
            a_pass(h, i)

    for j in range(nz):
        forward(j)
    p_wait(True)
    overlap(0)
    rows_sent()
    for i in range(nz):
        across(i, drain=True)
    for i in range(1, nz - 1):
        @pl.loop(0, nch)
        def _(h):
            a_last(h, i)
    a_last(0, nz - 1)

    a_ready(0)
    grow(0, k)

    for other in range(1, states):
        peer = lax.rem(k + other, states)
        ref = mbuf.at[peer]
        remote(ref, ref, mx_send, mx_recv.at[peer], peer, me).wait_recv()

    grow_others(0)
    overlap(1)
    for n in range(slices - 2):
        hand_over(nz - 2, n)
        hand_over(nz - 1, n)

    if nch > 1:
        a_last(1, nz - 1)

    @pl.loop(1, nch)
    def _(h):
        a_ready(h)
        grow_all(h)

        @pl.when(h < nch - 1)
        def _():
            a_last(h + 1, nz - 1)

        if direct:
            @pl.when(h > 1)
            def _():
                finish(h - 2)

    hand_over(nz - 2, slices - 2)
    hand_over(nz - 1, slices - 2)
    overlap(2)
    if direct:
        pass_on(0)
        finish(nch - 2)
        hand_over(nz - 2, slices - 1)
        hand_over(nz - 1, slices - 1)
        for h in range(1, nch - 2):
            pass_on(h)
        finish(nch - 1)
        for h in range(max(nch - 2, 1), nch):
            pass_on(h)
    else:
        hand_over(nz - 2, slices - 1)
        hand_over(nz - 1, slices - 1)


        @pl.loop(0, mine)
        def _(zc):
            finish(zc)

        @pl.loop(0, mine)
        def _(zc):
            pass_on(zc)

    penalize()
    for i in range(nz):
        a_edges(i, drain=True)
    a_sibling(drain=True)

    @pl.loop(0, nch)
    def _(h):
        for i in range(1, nz):
            a_pass(h, i, drain=True)
            a_last(h, i, drain=True)

    for i in range(nz):
        forward(i, drain=True)
        for n in range(slices):
            hand_over(i, n, drain=True)

    @pl.loop(0, nz)
    def _(zz):
        for u in range(1, ny):
            my_copy(zz, lax.rem(y + u, ny)).wait_send()
        for other in range(1, states):
            mx_copy(zz, y, lax.rem(k + other, states)).wait_send()

    share(drain=True)
    for send, number, _ in stages:
        for u in range(1, number):
            send(u).wait_send()

    @pl.loop(0, mine)
    def _(zc):
        for u in range(1, ny):
            for kk in range(states):
                t_copy(zc, lax.rem(y + u, ny), kk).wait_send()
        for kk in range(states):
            @pl.when(kk != k)
            def _():
                r_copy(kk, zc).wait_send()

            deliver(kk, zc, drain=True)

    if direct:
        rest = next_ref.at[:, pl.ds(0, (bonds - ny) * w)]
    else:
        rest = next_ref.at[pl.ds(0, bonds - ny)]
    remote(rest, rest, n_send, n_recv, k, me).wait_recv()


def shards(states, bonds, intersect_left, stored_block, stored_site, current_site, current_block, penalty_weight):
    rows, width = intersect_left.shape[1:]
    pairs, w = stored_block.shape[1:3]
    phys = stored_site.shape[1]
    fwidth = current_site.shape[2]
    groups = width // TILE
    gpp = groups // states
    ny = 1
    while 4 * ny * ny <= bonds // CORES:
        ny *= 2
    nz = bonds // (CORES * ny)
    direct = w % 128 == 0
    fch = ny * w if direct else max(w, 128)
    nch, mine = fwidth // fch, fwidth // w // ny
    cell = CORES * rows
    piece = phys * cell
    bf, f32 = jnp.bfloat16, jnp.float32
    anywhere = pl.BlockSpec(memory_space=pltpu.HBM)
    dma = pltpu.SemaphoreType.DMA
    penalized, grown = pl.pallas_call(
        functools.partial(kernel, states, bonds, ny, fch),
        out_shape=(
            pltpu.VMEM(current_block.shape, f32),
            pltpu.VMEM((w, bonds * w) if direct else (bonds, w, w), bf),
        ),
        in_specs=[anywhere] * 5 + [pl.BlockSpec(memory_space=pltpu.SMEM)],
        out_specs=(pl.BlockSpec(memory_space=pltpu.VMEM),) * 2,
        scratch_shapes=[
            pltpu.VMEM((bonds, PARTS, rows // PARTS, width), bf),
            pltpu.VMEM((rows, phys, fwidth), bf),
            pltpu.VMEM((nch, nz, phys, CORES, rows, fch), bf),
            pltpu.VMEM(((pairs + phys) * w, width), bf),
            pltpu.VMEM((groups, pairs, w, TILE), bf),
            pltpu.VMEM((groups, PARTS, pairs * w // PARTS, TILE), bf),
            pltpu.VMEM((states, gpp, PARTS, pairs * w // PARTS, TILE), bf),
            pltpu.VMEM((nz, ny, w, piece), bf),
            pltpu.VMEM((states, ny, w, nz * piece), bf),
            pltpu.VMEM((mine, states, ny * w, w), f32),
            pltpu.VMEM((mine, ny, states, ny * w, w), bf),
            pltpu.VMEM((mine, ny, states, ny * w, w), bf),
            pltpu.VMEM((states, mine, ny, w, w), bf),
            pltpu.VMEM((states, mine, ny, w, w), bf),
            pltpu.VMEM((CORES * ny, states, 128), f32),
            pltpu.VMEM((nz, states, 128), f32),
            pltpu.VMEM((states, states, 128), f32),
            pltpu.VMEM((states, 8, TILE), f32),
            dma((4,)),
            dma, dma((bonds, PARTS)),
            dma, dma((nch, nz, CORES)),
            dma, dma((states, nz)),
            dma, dma((nz, ny)),
            dma, dma((states,)),
            dma, dma,
            dma((3,)), dma((3,)),
            dma, dma((mine, ny, states)),
            dma, dma((states, mine)),
            dma, dma,
        ],
        compiler_params=pltpu.CompilerParams(
            collective_id=0, has_side_effects=True, vmem_limit_bytes=60 * 1024 * 1024
        ),
    )(
        intersect_left.reshape(PARTS, rows // PARTS, width), stored_block[0], stored_site[0],
        current_site, current_block, penalty_weight,
    )
    if direct:
        return penalized, grown[None]
    return penalized, grown.transpose(1, 0, 2).reshape(1, w, bonds * w)


def solution(mesh):
    placed = (
        P("state", "bond", None),
        P("state", None, "bond", None),
        P("state", None, "bond", None),
        P("bond", None, "state"),
        P(None, "bond", "state"),
        P(),
    )
    return jax.shard_map(
        functools.partial(shards, mesh.shape["state"], mesh.shape["bond"]),
        mesh=mesh,
        in_specs=placed,
        out_specs=(P(None, "bond", "state"), P("state", "bond", None)),
        check_vma=False,
    )
```

```python
import functools

import jax
import jax.numpy as jnp
from jax import lax
from jax.experimental import pallas as pl
from jax.experimental.pallas import tpu as pltpu
from jax.sharding import PartitionSpec as P

MESH = pl.DeviceIdType.MESH
CORES = 2
TILE = 256
PARTS = 2


def both(*conds):
    return functools.reduce(jnp.logical_and, conds)


def kernel(
    states, bonds, rows_y, fch,
    env_hbm, block_hbm, site_hbm, grow_hbm, current_hbm, weight_ref,
    pen_ref, next_ref,
    ebuf, raw, abuf, stored, cbuf, psend, precv, mown, mbuf, acc, part, prt, nsend, nbuf, iplane, iline, istate, line,
    local_sem, e_send, e_recv, a_send, a_recv, p_send, p_recv, my_send, my_recv, mx_send, mx_recv,
    c_send, c_recv, i_send, i_recv, t_send, t_recv, r_send, r_recv, n_send, n_recv,
):
    nc, ny = CORES, rows_y
    nz = bonds // (nc * ny)
    hr, width = ebuf.shape[2:]
    rows = hr * PARTS
    pairs, w = block_hbm.shape[:2]
    phys = site_hbm.shape[0]
    fwidth = grow_hbm.shape[2]
    nch = fwidth // fch
    bpc = fch // w
    fbs = fwidth // w
    mine = fbs // ny
    cell = nc * rows
    per_group = TILE // rows
    tpp = ny * cell // TILE
    cpt = TILE // cell
    groups = width // TILE
    gpp = groups // states
    ecols = states * ny * w
    direct = w % 128 == 0
    piece = phys * cell

    k = lax.axis_index("state")
    me = lax.axis_index("bond")
    c = lax.rem(me, nc)
    y = lax.rem(lax.div(me, nc), ny)
    z = lax.div(me, nc * ny)
    near = ny * nc
    slices = PARTS * tpp

    def slot(zz, yy, cc):
        return (zz * ny + yy) * nc + cc

    sib = slot(z, y, 1 - c)

    def owner_of(zz):
        return lax.div(zz * tpp, gpp)

    def order(kk, zz):
        rest = sorted(set(range(nz)) - {zz}, key=lambda other: abs(other - zz))
        return [zz] + sorted(rest, key=lambda other: other * tpp // gpp == kk)

    def turn_of(kk, j):
        at = jnp.int32(0)
        for k_ in range(states):
            for z_ in range(nz):
                at = at + jnp.where(both(kk == k_, z == z_), order(k_, z_)[j], 0)
        return at

    turns = [turn_of(k, j) for j in range(nz)]

    def turn(j):
        return turns[j]

    def column_of(h, q):
        if direct:
            return (h // nc * ny + q) * nc + h % nc
        return h * bpc + q

    e_load = pltpu.make_async_copy(env_hbm, ebuf.at[me], local_sem.at[0])
    e_load.start()
    a_load = pltpu.make_async_copy(grow_hbm, raw, local_sem.at[1])
    a_load.start()
    loads = []
    for q in range(pairs):
        loads.append(pltpu.make_async_copy(block_hbm.at[q], stored.at[pl.ds(q * w, w)], local_sem.at[2]))
    for s in range(phys):
        loads.append(
            pltpu.make_async_copy(site_hbm.at[s], stored.at[pl.ds((pairs + s) * w, w)], local_sem.at[2])
        )
    for copy in loads:
        copy.start()
    c_loads = [
        pltpu.make_async_copy(
            current_hbm.at[:, :, pl.ds(g * TILE, TILE)], cbuf.at[k * gpp + g], local_sem.at[3]
        )
        for g in range(gpp)
    ]
    for copy in c_loads:
        copy.start()

    barrier = pltpu.get_barrier_semaphore()

    def greet(kk, dest):
        pl.semaphore_signal(barrier, inc=1, device_id=(kk, dest), device_id_type=MESH)

    @pl.when(z > 0)
    def _():
        greet(k, slot(z - 1, y, c))

    @pl.when(z < nz - 1)
    def _():
        greet(k, slot(z + 1, y, c))

    for other in range(1, near):
        greet(k, z * near + lax.rem(lax.rem(me, near) + other, near))
    for other in range(1, states):
        greet(lax.rem(k + other, states), me)
    ends = jnp.where(z > 0, 1, 0) + jnp.where(z < nz - 1, 1, 0)
    pl.semaphore_wait(barrier, near + states - 2 + ends)

    def remote(src, dst, ss, rs, kk, dest):
        return pltpu.make_async_remote_copy(
            src_ref=src, dst_ref=dst, send_sem=ss, recv_sem=rs, device_id=(kk, dest), device_id_type=MESH
        )

    def act(copy, drain):
        if drain:
            copy.wait_send()
        else:
            copy.start()


    def e_copy(blk, h, dest):
        ref = ebuf.at[blk, h]
        return remote(ref, ref, e_send, e_recv.at[blk, h], k, dest)

    def spread(blk, h, drain=False):
        @pl.when(y > 0)
        def _():
            act(e_copy(blk, h, slot(z, y - 1, c)), drain)

        @pl.when(y < ny - 1)
        def _():
            act(e_copy(blk, h, slot(z, y + 1, c)), drain)

    def within(zz):
        return both(zz >= 0, zz < nz)


    def late(zz, sign):
        return both(owner_of(zz) == k, k != (0 if sign > 0 else states - 1))

    def pass_z(zz, h, sign, drain=False):
        @pl.when(within(z + sign))
        def _():
            act(e_copy(slot(zz, y, c), h, slot(z + sign, y, c)), drain)

    def own():
        for h in range(PARTS):
            for sign in (1, -1):
                if h < PARTS - 1:
                    pass_z(z, h, sign)
                else:
                    @pl.when(jnp.logical_not(late(z, sign)))
                    def _():
                        pass_z(z, h, sign)
            spread(me, h)
            act(e_copy(me, h, sib), False)

    def own_late(sign):
        @pl.when(late(z, sign))
        def _():
            pass_z(z, PARTS - 1, sign)

    def take(zz, h, sign):
        blk = slot(zz, y, c)
        e_copy(blk, h, me).wait_recv()
        pass_z(zz, h, sign)
        act(e_copy(blk, h, sib), False)

    reach = jnp.maximum(jnp.where(k > 0, z, 0), jnp.where(k < states - 1, nz - 1 - z, 0))

    def natural(i, wanted, parts=range(PARTS)):
        for h in parts:
            for sign in (1, -1):
                zz = z - sign * i
                kept = owner_of(zz) == k
                mine_now = kept if wanted else jnp.logical_not(kept)
                if wanted and h == PARTS - 1:
                    mine_now = both(mine_now, jnp.logical_not(late(zz, sign)))

                @pl.when(both(within(zz), mine_now))
                def _():
                    take(zz, h, sign)
                    if wanted and i < nz - 2:
                        @pl.when(jnp.logical_or(late(zz, sign), reach <= i))
                        def _():
                            spread(slot(zz, y, c), h)
                    else:
                        spread(slot(zz, y, c), h)

    def deferred():
        for i in range(1, nz - 2):
            for sign in (1, -1):
                zz = z - sign * i

                @pl.when(both(within(zz), owner_of(zz) == k, reach > i, jnp.logical_not(late(zz, sign))))
                def _():
                    for h in range(PARTS):
                        spread(slot(zz, y, c), h)

    def delayed():
        for i in range(1, nz):
            for sign in (1, -1):
                zz = z - sign * i

                @pl.when(both(within(zz), late(zz, sign)))
                def _():
                    take(zz, PARTS - 1, sign)
                    spread(slot(zz, y, c), PARTS - 1)

    def rows_sent():
        for h in range(PARTS):
            for i in range(nz):
                for sign in (1, -1):
                    zz = z - sign * i

                    @pl.when(within(zz))
                    def _():
                        pass_z(zz, h, sign, drain=True)
                        if i or sign > 0:
                            spread(slot(zz, y, c), h, drain=True)
                            act(e_copy(slot(zz, y, c), h, sib), True)

    def across(j, drain=False):
        zz = turn(j)
        for h in range(PARTS):
            for u in range(1, ny):
                for sign in (1, -1):
                    yy = y - sign * u
                    onward = y + sign

                    @pl.when(both(yy >= 0, yy < ny))
                    def _():
                        blk = slot(zz, yy, c)
                        if not drain:
                            e_copy(blk, h, me).wait_recv()

                        @pl.when(both(onward >= 0, onward < ny))
                        def _():
                            act(e_copy(blk, h, slot(z, onward, c)), drain)

                        act(e_copy(blk, h, sib), drain)

    def sibling(j):
        zz = turn(j)
        for h in range(PARTS):
            for yy in range(ny):
                e_copy(slot(zz, yy, 1 - c), h, me).wait_recv()


    def unpack():
        for s in range(phys):
            plain = raw[:, s, :]
            for h in range(nch):
                for q in range(bpc):
                    at = column_of(h, q) * w
                    abuf[h, z, s, c, :, q * w : (q + 1) * w] = plain[:, at : at + w]

    def a_copy(h, zz, cc, dest):
        ref = abuf.at[h, zz, :, cc]
        return remote(ref, ref, a_send, a_recv.at[h, zz, cc], k, dest)

    def a_own(sign, drain=False):
        @pl.loop(0 if drain else jnp.where(late(z, sign), 1, 0), nch)
        def _(h):
            act(a_copy(h, z, c, slot(z + sign, y, c)), drain)

    def a_first():
        for sign in (1, -1):
            @pl.when(both(within(z + sign), late(z, sign)))
            def _():
                a_copy(0, z, c, slot(z + sign, y, c)).start()

    def a_edges(i, drain=False):
        @pl.when(both(z == i, z < nz - 1))
        def _():
            if not drain:
                own_late(1)
            a_own(1, drain)

        @pl.when(both(nz - 1 - z == i, z > 0))
        def _():
            if not drain:
                own_late(-1)
            a_own(-1, drain)

    def a_sibling(drain=False):
        @pl.loop(0, nch)
        def _(h):
            act(a_copy(h, z, c, sib), drain)

    def a_pass(h, i, drain=False):
        for sign in (1, -1):
            zz = z - sign * i
            onward = z + sign

            @pl.when(both(zz >= 0, zz < nz, onward >= 0, onward < nz))
            def _():
                if not drain:
                    a_copy(h, zz, c, me).wait_recv()
                act(a_copy(h, zz, c, slot(onward, y, c)), drain)
                act(a_copy(h, zz, c, sib), drain)

    def a_last(h, i, drain=False):
        for sign in (1, -1):
            zz = z - sign * i
            onward = z + sign

            @pl.when(both(zz >= 0, zz < nz, jnp.logical_or(onward < 0, onward >= nz)))
            def _():
                if not drain:
                    a_copy(h, zz, c, me).wait_recv()
                act(a_copy(h, zz, c, sib), drain)

    def a_ready(h):
        for zz in range(nz):
            a_copy(h, zz, 1 - c, me).wait_recv()


    def c_copy(zz, peer):
        ref = cbuf.at[pl.ds(zz * tpp, tpp)]
        return remote(ref, ref, c_send, c_recv, peer, me)

    def share(drain=False):
        for other in range(1, states):
            peer = lax.rem(k + other, states)
            zz = turn_of(peer, nz - 2)

            @pl.when(owner_of(zz) == k)
            def _():
                act(c_copy(zz, peer), drain)


    def p_copy(g, part_of, peer):
        return remote(
            psend.at[g, part_of], precv.at[k, lax.rem(g, gpp), part_of],
            p_send, p_recv.at[k, lax.div(g, tpp)], peer, me,
        )

    def span(zz):
        return pl.ds(pl.multiple_of(zz * piece, 128), piece)

    def my_copy(zz, yy):
        return remote(
            mown.at[zz, yy], mbuf.at[k, y, :, span(zz)], my_send, my_recv.at[zz, y], k, slot(z, yy, c)
        )

    def mx_copy(zz, yy, peer):
        ref = mbuf.at[k, yy, :, span(zz)]
        return remote(ref, ref, mx_send, mx_recv.at[k], peer, me)

    def flat_of(kk, at):
        return precv[kk, at].reshape(pairs * w, TILE).astype(jnp.float32)

    def halves(whole):
        return whole.astype(jnp.bfloat16).reshape(PARTS, pairs * w // PARTS, TILE)

    def tally(kk, g, whole):
        here = cbuf[g].reshape(pairs * w, TILE).astype(jnp.float32)
        line[kk] += jnp.sum((whole * here).reshape(pairs * w // 8, 8, TILE), axis=0)

    def p_wait(use):
        for i in range(nz // states):
            zz = k * (nz // states) + i
            for other in range(1, states):
                peer = lax.rem(k + other, states)
                counted = zz == turn_of(peer, nz - 2)

                @pl.when(jnp.logical_not(counted) if use else counted)
                def _():
                    ref = precv.at[peer, pl.ds(i * tpp, tpp)]
                    remote(ref, ref, p_send, p_recv.at[peer, zz], peer, me).wait_recv()
                    if use:
                        @pl.loop(0, tpp)
                        def _(r):
                            tally(peer, zz * tpp + r, flat_of(peer, i * tpp + r))

    def project(j):
        zz = turn(j)

        if j == nz - 2:
            @pl.when(owner_of(zz) != k)
            def _():
                c_copy(zz, k).wait_recv()

        @pl.loop(0, tpp)
        def _(r):
            g = zz * tpp + r
            left = ebuf[pl.ds(g * per_group, per_group)].reshape(TILE, width)
            prod = lax.dot_general(
                stored[...], left, (((1,), (1,)), ((), ())), preferred_element_type=jnp.float32
            )
            for q in range(cpt):
                yy = r * cpt + q
                moved = jnp.concatenate(
                    [
                        prod[(pairs + s) * w : (pairs + s + 1) * w, q * cell : (q + 1) * cell]
                        for s in range(phys)
                    ],
                    axis=1,
                ).astype(jnp.bfloat16)

                @pl.when(yy == y)
                def _():
                    mbuf[k, y, :, span(zz)] = moved
                    for other in range(1, states):
                        mx_copy(zz, y, lax.rem(k + other, states)).start()

                @pl.when(yy != y)
                def _():
                    mown[zz, yy] = moved
                    if j >= nz - 2:
                        my_copy(zz, yy).start()

            whole = prod[: pairs * w]
            owner = lax.div(g, gpp)

            @pl.when(jnp.logical_or(owner == k, j == nz - 2))
            def _():
                tally(k, g, whole)

            @pl.when(owner == k)
            def _():
                precv[k, lax.rem(g, gpp)] = halves(whole)

            @pl.when(owner != k)
            def _():
                psend[g] = halves(whole)

    def hand_over(j, n, drain=False):
        zz = turn(j)
        g = zz * tpp + n // PARTS
        for other in range(1, states):
            peer = lax.rem(k + other, states)

            @pl.when(lax.div(g, gpp) == peer)
            def _():
                act(p_copy(g, n % PARTS, peer), drain)

    def forward(j, drain=False):
        zz = turn(j)
        for u in range(1, ny):
            yy = lax.rem(y + u, ny)
            if not drain:
                ref = mbuf.at[k, yy, :, span(zz)]
                remote(ref, ref, my_send, my_recv.at[zz, yy], k, me).wait_recv()
            for other in range(1, states):
                act(mx_copy(zz, yy, lax.rem(k + other, states)), drain)


    def t_copy(zc, yy, kk):
        return remote(
            part.at[zc, yy, kk], prt.at[zc, y, kk], t_send, t_recv.at[zc, y, kk], k, slot(z, yy, c)
        )

    def parts_of(h):
        for q in range(bpc):
            if direct:
                yield q, h, q
            else:
                fb = h * bpc + q
                yield (
                    q,
                    lax.div(fb, ny * nc) * nc + lax.rem(fb, nc),
                    lax.rem(lax.div(fb, nc), ny),
                )

    def store(zc, yy, kk, block):
        @pl.when(yy == y)
        def _():
            acc[zc, kk] = block

        @pl.when(yy != y)
        def _():
            part[zc, yy, kk] = block.astype(jnp.bfloat16)

    def grow(h, kk):
        total = jnp.dot(
            mbuf[kk].reshape(ny * w, nz * piece),
            abuf[h].reshape(nz * piece, fch),
            preferred_element_type=jnp.float32,
        )
        for q, zc, yy in parts_of(h):
            store(zc, yy, kk, total[:, q * w : (q + 1) * w])

            @pl.when(yy != y)
            def _():
                t_copy(zc, yy, kk).start()

    def grow_all(h):
        total = jnp.dot(
            mbuf[...].reshape(ecols, nz * piece),
            abuf[h].reshape(nz * piece, fch),
            preferred_element_type=jnp.float32,
        )
        for q, zc, yy in parts_of(h):
            for kk in range(states):
                store(zc, yy, kk, total[kk * ny * w : (kk + 1) * ny * w, q * w : (q + 1) * w])

            @pl.when(yy != y)
            def _():
                for other in range(1, states + 1):
                    t_copy(zc, yy, lax.rem(k + other, states)).start()

    def grow_others(h):
        @pl.loop(1, states)
        def _(other):
            grow(h, lax.rem(k + other, states))

    def target(kk, zc):
        return slot(kk * (nz // states) + lax.div(zc, nc), y, lax.rem(zc, nc))

    def place(src):
        if direct:
            return next_ref.at[:, pl.ds(pl.multiple_of(src * w, 128), w)]
        return next_ref.at[src]


    def n_copy(kk, zc, yy):
        return remote(
            nbuf.at[kk, zc, yy], place(slot(z, yy, c)), n_send, n_recv, k, target(kk, zc)
        )

    def deliver(kk, zc, drain=False):
        stays = target(kk, zc) == me
        for yy in range(ny):
            if not drain:
                @pl.when(stays)
                def _():
                    place(slot(z, yy, c))[...] = nbuf[kk, zc, yy]

            @pl.when(jnp.logical_not(stays))
            def _():
                act(n_copy(kk, zc, yy), drain)

    def r_copy(kk, zc):
        return remote(nsend.at[kk, zc], nbuf.at[k, zc], r_send, r_recv.at[k, zc], kk, me)

    def summed(zc, kk):
        total = acc[zc, kk]
        for u in range(1, ny):
            yy = lax.rem(y + u, ny)
            ref = prt.at[zc, yy, kk]
            remote(ref, ref, t_send, t_recv.at[zc, yy, kk], k, me).wait_recv()
            total = total + ref[...].astype(jnp.float32)
        return [total[yy * w : (yy + 1) * w].T.astype(jnp.bfloat16) for yy in range(ny)]

    def finish(zc):
        for other in range(1, states):
            kk = lax.rem(k + other, states)
            blocks = summed(zc, kk)
            for yy in range(ny):
                nsend[kk, zc, yy] = blocks[yy]
            r_copy(kk, zc).start()
        blocks = summed(zc, k)
        for yy in range(ny):
            nbuf[k, zc, yy] = blocks[yy]
        deliver(k, zc)

    def pass_on(zc):
        for other in range(1, states):
            kk = lax.rem(k + other, states)
            ref = nbuf.at[kk, zc]
            remote(ref, ref, r_send, r_recv.at[kk, zc], k, me).wait_recv()
            deliver(kk, zc)


    def i_near(u):
        there = lax.rem(lax.rem(me, near) + u, near)
        ref = iplane.at[lax.rem(me, near)]
        return remote(ref, ref, i_send.at[0], i_recv.at[0], k, z * near + there)

    def i_far(u):
        ref = iline.at[z]
        return remote(ref, ref, i_send.at[1], i_recv.at[1], k, slot(lax.rem(z + u, nz), y, c))

    def i_peer(u):
        ref = istate.at[k]
        return remote(ref, ref, i_send.at[2], i_recv.at[2], lax.rem(k + u, states), me)

    stages = ((i_near, near, iplane), (i_far, nz, iline), (i_peer, states, istate))

    def start(n):
        send, number, _ = stages[n]
        for u in range(1, number):
            send(u).start()

    def gathered(n):
        _, number, buf = stages[n]
        rest = buf.at[pl.ds(0, number - 1)]
        remote(rest, rest, i_send.at[n], i_recv.at[n], k, me).wait_recv()

    def overlap(n):
        if n == 0:
            for kk in range(states):
                short = jnp.sum(line[kk], axis=0, keepdims=True)
                total = short[:, :128]
                for at in range(128, TILE, 128):
                    total = total + short[:, at : at + 128]
                iplane[lax.rem(me, near), kk : kk + 1] = total
        elif n == 1:
            gathered(0)
            iline[z] = jnp.sum(iplane[...], axis=0)
        else:
            gathered(1)
            istate[k] = jnp.sum(iline[...], axis=0)
        start(n)

    def penalize():
        gathered(2)
        p_wait(False)
        scale = 1.0 / (phys * width)
        factors = [weight_ref[kk] * (jnp.sum(istate[:, kk]) * scale) for kk in range(states)]
        for g in range(gpp):
            value = cbuf[k * gpp + g].reshape(pairs * w, TILE).astype(jnp.float32)
            for kk in range(states):
                value = value + factors[kk] * flat_of(kk, g)
            pen_ref[:, :, g * TILE : (g + 1) * TILE] = value.reshape(pairs, w, TILE)

    line[...] = jnp.zeros_like(line)
    e_load.wait()
    for i in range(nz + 1):
        if i == 0:
            own()
            a_load.wait()
            unpack()
            a_first()
            a_sibling()
        elif i < nz:
            if i < nz - 1:
                natural(i, False)
            if i == nz - 2:
                natural(nz - 1, False, range(PARTS - 1))
                for u in range(1, ny):
                    my_copy(turn(0), lax.rem(y + u, ny)).start()
                deferred()
            if i == nz - 1:
                natural(nz - 1, False, [PARTS - 1])
            natural(i, True)
            if i == nz - 1:
                delayed()
        if i < nz:
            a_edges(i)
            if i == 0:
                for copy in c_loads:
                    copy.wait()
                share()
        if i == nz - 1:
            for j in range(1, nz - 2):
                for u in range(1, ny):
                    my_copy(turn(j), lax.rem(y + u, ny)).start()

            @pl.loop(0, nch)
            def _(h):
                a_pass(h, 1)
        if i >= 1:
            across(i - 1)
            sibling(i - 1)
            if i == 1:
                for copy in loads:
                    copy.wait()
            project(i - 1)
            if i == nz - 1:
                forward(0)
            if i - 1 < nz - 2:
                for n in range(slices):
                    hand_over(i - 1, n)

    for i in range(2, nz):
        @pl.loop(0, nch)
        def _(h):
            a_pass(h, i)

    for j in range(1, nz):
        forward(j)
    p_wait(True)
    overlap(0)
    rows_sent()
    for i in range(nz):
        across(i, drain=True)
    for i in range(1, nz - 1):
        @pl.loop(0, nch)
        def _(h):
            a_last(h, i)
    a_last(0, nz - 1)

    a_ready(0)
    grow(0, k)

    for other in range(1, states):
        peer = lax.rem(k + other, states)
        ref = mbuf.at[peer]
        remote(ref, ref, mx_send, mx_recv.at[peer], peer, me).wait_recv()

    grow_others(0)
    overlap(1)
    for n in range(slices - 2):
        hand_over(nz - 2, n)
        hand_over(nz - 1, n)

    if nch > 1:
        a_last(1, nz - 1)

    @pl.loop(1, nch)
    def _(h):
        a_ready(h)
        grow_all(h)

        @pl.when(h < nch - 1)
        def _():
            a_last(h + 1, nz - 1)

        if direct:
            @pl.when(h > 1)
            def _():
                finish(h - 2)

    hand_over(nz - 2, slices - 2)
    hand_over(nz - 1, slices - 2)
    overlap(2)
    if direct:
        pass_on(0)
        finish(nch - 2)
        hand_over(nz - 2, slices - 1)
        hand_over(nz - 1, slices - 1)
        for h in range(1, nch - 2):
            pass_on(h)
        finish(nch - 1)
        for h in range(max(nch - 2, 1), nch):
            pass_on(h)
    else:
        hand_over(nz - 2, slices - 1)
        hand_over(nz - 1, slices - 1)


        @pl.loop(0, mine)
        def _(zc):
            finish(zc)

        @pl.loop(0, mine)
        def _(zc):
            pass_on(zc)

    penalize()
    for i in range(nz):
        a_edges(i, drain=True)
    a_sibling(drain=True)

    @pl.loop(0, nch)
    def _(h):
        for i in range(1, nz):
            a_pass(h, i, drain=True)
            a_last(h, i, drain=True)

    for i in range(nz):
        forward(i, drain=True)
        for n in range(slices):
            hand_over(i, n, drain=True)

    @pl.loop(0, nz)
    def _(zz):
        for u in range(1, ny):
            my_copy(zz, lax.rem(y + u, ny)).wait_send()
        for other in range(1, states):
            mx_copy(zz, y, lax.rem(k + other, states)).wait_send()

    share(drain=True)
    for send, number, _ in stages:
        for u in range(1, number):
            send(u).wait_send()

    @pl.loop(0, mine)
    def _(zc):
        for u in range(1, ny):
            for kk in range(states):
                t_copy(zc, lax.rem(y + u, ny), kk).wait_send()
        for kk in range(states):
            @pl.when(kk != k)
            def _():
                r_copy(kk, zc).wait_send()

            deliver(kk, zc, drain=True)

    if direct:
        rest = next_ref.at[:, pl.ds(0, (bonds - ny) * w)]
    else:
        rest = next_ref.at[pl.ds(0, bonds - ny)]
    remote(rest, rest, n_send, n_recv, k, me).wait_recv()


def shards(states, bonds, intersect_left, stored_block, stored_site, current_site, current_block, penalty_weight):
    rows, width = intersect_left.shape[1:]
    pairs, w = stored_block.shape[1:3]
    phys = stored_site.shape[1]
    fwidth = current_site.shape[2]
    groups = width // TILE
    gpp = groups // states
    ny = 1
    while 4 * ny * ny <= bonds // CORES:
        ny *= 2
    nz = bonds // (CORES * ny)
    direct = w % 128 == 0
    fch = ny * w if direct else max(w, 128)
    nch, mine = fwidth // fch, fwidth // w // ny
    cell = CORES * rows
    piece = phys * cell
    bf, f32 = jnp.bfloat16, jnp.float32
    anywhere = pl.BlockSpec(memory_space=pltpu.HBM)
    dma = pltpu.SemaphoreType.DMA
    penalized, grown = pl.pallas_call(
        functools.partial(kernel, states, bonds, ny, fch),
        out_shape=(
            pltpu.VMEM(current_block.shape, f32),
            pltpu.VMEM((w, bonds * w) if direct else (bonds, w, w), bf),
        ),
        in_specs=[anywhere] * 5 + [pl.BlockSpec(memory_space=pltpu.SMEM)],
        out_specs=(pl.BlockSpec(memory_space=pltpu.VMEM),) * 2,
        scratch_shapes=[
            pltpu.VMEM((bonds, PARTS, rows // PARTS, width), bf),
            pltpu.VMEM((rows, phys, fwidth), bf),
            pltpu.VMEM((nch, nz, phys, CORES, rows, fch), bf),
            pltpu.VMEM(((pairs + phys) * w, width), bf),
            pltpu.VMEM((groups, pairs, w, TILE), bf),
            pltpu.VMEM((groups, PARTS, pairs * w // PARTS, TILE), bf),
            pltpu.VMEM((states, gpp, PARTS, pairs * w // PARTS, TILE), bf),
            pltpu.VMEM((nz, ny, w, piece), bf),
            pltpu.VMEM((states, ny, w, nz * piece), bf),
            pltpu.VMEM((mine, states, ny * w, w), f32),
            pltpu.VMEM((mine, ny, states, ny * w, w), bf),
            pltpu.VMEM((mine, ny, states, ny * w, w), bf),
            pltpu.VMEM((states, mine, ny, w, w), bf),
            pltpu.VMEM((states, mine, ny, w, w), bf),
            pltpu.VMEM((CORES * ny, states, 128), f32),
            pltpu.VMEM((nz, states, 128), f32),
            pltpu.VMEM((states, states, 128), f32),
            pltpu.VMEM((states, 8, TILE), f32),
            dma((4,)),
            dma, dma((bonds, PARTS)),
            dma, dma((nch, nz, CORES)),
            dma, dma((states, nz)),
            dma, dma((nz, ny)),
            dma, dma((states,)),
            dma, dma,
            dma((3,)), dma((3,)),
            dma, dma((mine, ny, states)),
            dma, dma((states, mine)),
            dma, dma,
        ],
        compiler_params=pltpu.CompilerParams(
            collective_id=0, has_side_effects=True, vmem_limit_bytes=60 * 1024 * 1024
        ),
    )(
        intersect_left.reshape(PARTS, rows // PARTS, width), stored_block[0], stored_site[0],
        current_site, current_block, penalty_weight,
    )
    if direct:
        return penalized, grown[None]
    return penalized, grown.transpose(1, 0, 2).reshape(1, w, bonds * w)


def solution(mesh):
    placed = (
        P("state", "bond", None),
        P("state", None, "bond", None),
        P("state", None, "bond", None),
        P("bond", None, "state"),
        P(None, "bond", "state"),
        P(),
    )
    return jax.shard_map(
        functools.partial(shards, mesh.shape["state"], mesh.shape["bond"]),
        mesh=mesh,
        in_specs=placed,
        out_specs=(P(None, "bond", "state"), P("state", "bond", None)),
        check_vma=False,
    )
```
